512 devices in a mesh: row: 32 (over x, y), shift: 16 (over z, core).
Axes of the slice: x: 4, y: 8, z: 8, core: 2. Of those that a mesh axis runs over, the one named last changes fastest.
Arguments:
- snapshots: bfloat16 [4096, 2, 128], P('row'), may hold values from -6 to 6
- tail_sensors: bfloat16 [128, 2, 128], replicated, may hold values from -6 to 6
- shift_offsets: int32 [48], P('shift'), may hold values from 0 to 128
- start_basis: float32 [64, 4096], P(None, 'row'), may hold values from -0.09375 to 0.09375
Outputs:
- covariance: float32 [4096, 4096], P('row', 'shift')
- signal_basis: float32 [64, 4096], P(None, 'row')
The draws below stay inside these ranges and needn't reach their ends.
Inputs may be any that keep to these rules, and one draw needn't show every extreme that they name: `shift_offsets`: each shift's first sensor.
All inputs are finite; a program needn't handle non-finite values.
Results may differ from the reference program's by a relative error of at most 0.0031.
Values may be sent and summed in bfloat16 or wider, within the bound.
A program may use at most 64 MiB of HBM per device.

```python
import jax
import jax.numpy as jnp
from jax import lax

M = 4096
K = 64
SNAPS = 128
TAIL = 128
ITERS = 2
SHIFTS = 48


def place_ends(drawn, stream_key, smallest, largest):
    longest = drawn.shape.index(max(drawn.shape))
    spots = []
    for shift in (0, 1):
        where = [jax.random.randint(jax.random.fold_in(stream_key, axis), (), 0, length) for axis, length in enumerate(drawn.shape)]
        where[longest] = (where[longest] + shift) % drawn.shape[longest]
        spots.append(tuple(where))
    return drawn.at[spots[0]].set(smallest).at[spots[1]].set(largest)


def level_of(rng, dims, split, low, high):
    factor_of, own = 1.0, jax.random.fold_in(rng, 6)
    for position, parts in split:
        draws = jnp.exp(jax.random.uniform(jax.random.fold_in(own, position), (parts,), jnp.float32, low / len(split), high / len(split)))
        factor_of = factor_of * jnp.repeat(draws, dims[position] // parts).reshape([-1 if axis == position else 1 for axis in range(len(dims))])
    return factor_of


def normal_values(stream_key, shape, scale, limit, split=(), held_as=jnp.bfloat16):
    factor_of = level_of(stream_key, shape, split, -0.22, 0.18) if split else 1.0
    entries = jax.random.normal(stream_key, shape, jnp.float32) * scale * factor_of
    return jnp.minimum(jnp.maximum(entries, -limit), limit).astype(held_as)


def setup_inputs(seed: int = 0) -> dict:
    splits = jax.random.split(jax.random.key(seed), 5)
    return {
        "snapshots": normal_values(splits[0], (M, 2, SNAPS), 0.7071, 6.0, ((0, 32),)),
        "tail_sensors": normal_values(splits[1], (TAIL, 2, SNAPS), 0.7071, 6.0),
        "shift_offsets": place_ends(jax.random.randint(splits[2], (SHIFTS,), 0, TAIL + 1), jax.random.fold_in(splits[2], 1), 0, TAIL).astype(jnp.int32),
        "start_basis": normal_values(splits[3], (K, M), M ** -0.5, 0.09375, ((1, 32),), jnp.float32),
    }


half_root = 0.7071067811865476

def make_rows(extended, offset):
    window = lax.dynamic_slice_in_dim(extended, offset, M, 0).astype(jnp.float32)
    mirror = window[::-1]
    summed_pair = window + mirror
    difference = window - mirror
    half_rows = M // 2
    upper_rows = jnp.concatenate([summed_pair[:half_rows, 0], summed_pair[:half_rows, 1]], axis=1)
    bottom = jnp.concatenate([difference[half_rows:, 1], -difference[half_rows:, 0]], axis=1)
    return (jnp.concatenate([upper_rows, bottom], 0) * half_root).astype(jnp.bfloat16)

def factor(gram_matrix):
    lower_factor = jnp.linalg.cholesky(gram_matrix)
    identity = jnp.eye(gram_matrix.shape[0], dtype=jnp.float32)
    return jax.scipy.linalg.solve_triangular(lower_factor, identity, lower=True)

def reference(snapshots, tail_sensors, shift_offsets, start_basis):
    extended = jnp.concatenate([snapshots, tail_sensors], 0)

    def add_shift(running, offset):
        pair_rows = make_rows(extended, offset)
        return (running + jnp.dot(pair_rows.astype(jnp.float32), pair_rows.T.astype(jnp.float32), preferred_element_type=jnp.float32), None)
    covariance_sum, unused = lax.scan(add_shift, jnp.zeros((M, M), jnp.float32), shift_offsets)
    covariance = covariance_sum * (1.0 / (SNAPS * SHIFTS))
    basis_rows = start_basis
    for sweep in range(ITERS):
        mapped = lax.dot_general(basis_rows, covariance, (((1,), (1,)), ((), ())), precision=lax.Precision.HIGHEST)
        gram_matrix = jnp.dot(mapped, mapped.T, precision=lax.Precision.HIGHEST)
        basis_rows = jnp.dot(factor(gram_matrix), mapped, precision=lax.Precision.HIGHEST)
    return (covariance, basis_rows)
```

```python
import jax
import jax.numpy as jnp
from jax import lax
from jax.experimental import pallas as pl
from jax.experimental.pallas import tpu as pltpu
from jax.sharding import PartitionSpec as P

M = 4096
K = 64
SNAPS = 128
SHIFTS = 48
ROWS = 32
COLS = 16
BLOCK = 128
HALF_ROOT = 0.7071067811865476
MESH = pl.DeviceIdType.MESH
HIGHEST = lax.Precision.HIGHEST
F32 = jnp.float32
BF16 = jnp.bfloat16


def signal_peers(barrier, r, t):
    def plane(k, _):
        pl.semaphore_signal(
            barrier, inc=1, device_id={"row": lax.rem(r + k, ROWS)}, device_id_type=MESH
        )
        return _

    def line(k, _):
        pl.semaphore_signal(
            barrier, inc=1, device_id={"shift": lax.rem(t + k, COLS)}, device_id_type=MESH
        )
        return _

    lax.fori_loop(1, ROWS, plane, 0)
    lax.fori_loop(1, COLS, line, 0)


def gather_kernel(own_ref, tail_ref, offs_ref, got_ref, offs_out, send_sem, near_sem, recv_sem, offs_send, offs_recv):
    r = lax.axis_index("row")
    t = lax.axis_index("shift")
    barrier = pltpu.get_barrier_semaphore()
    signal_peers(barrier, r, t)
    pl.semaphore_wait(barrier, ROWS - 1 + COLS - 1)

    def block_copy(slot, dest, send):
        return pltpu.make_async_remote_copy(
            src_ref=own_ref,
            dst_ref=got_ref.at[slot],
            send_sem=send,
            recv_sem=recv_sem.at[slot],
            device_id={"row": dest},
            device_id_type=MESH,
        )

    firsts = (2 * t, 30 - 2 * t)
    for group, first in enumerate(firsts):
        place = r - first

        @pl.when((place >= 0) & (place <= 2))
        def _():
            slot = 3 + 3 * group + place

            def send(k, c):
                block_copy(slot, lax.rem(r + k, ROWS), send_sem.at[group, k]).start()
                return c

            lax.fori_loop(1, ROWS, send, 0)
            got_ref[slot] = own_ref[...]

    @pl.when(r >= 1)
    def _():
        block_copy(0, r - 1, near_sem.at[0]).start()

    block_copy(1, 31 - r, near_sem.at[1]).start()

    @pl.when((r >= 1) & (r != 16))
    def _():
        block_copy(2, 32 - r, near_sem.at[2]).start()

    def offs_copy(k):
        return pltpu.make_async_remote_copy(
            src_ref=offs_ref,
            dst_ref=offs_out.at[t],
            send_sem=offs_send,
            recv_sem=offs_recv,
            device_id={"shift": lax.rem(t + k, COLS)},
            device_id_type=MESH,
        )

    def send_offs(k, c):
        offs_copy(k).start()
        return c

    lax.fori_loop(1, COLS, send_offs, 0)
    offs_out[t] = offs_ref[...]

    @pl.when(r == 31)
    def _():
        got_ref[0] = tail_ref[...]

    @pl.when(r == 0)
    def _():
        got_ref[2] = tail_ref[...]

    @pl.when(r == 16)
    def _():
        got_ref[2] = own_ref[...]

    @pl.when(t == 15)
    def _():
        got_ref[5] = tail_ref[...]

    @pl.when(t == 0)
    def _():
        got_ref[8] = tail_ref[...]

    def arrived(slot):
        block_copy(slot, r, near_sem.at[0]).wait_recv()

    @pl.when(r != 31)
    def _():
        arrived(0)

    arrived(1)

    @pl.when((r != 0) & (r != 16))
    def _():
        arrived(2)

    for group, first in enumerate(firsts):
        for place in range(3):
            block = first + place

            @pl.when((block != r) & (block != 32))
            def _():
                arrived(3 + 3 * group + place)

    every = offs_out.at[pl.ds(0, COLS - 1)]
    whole = pltpu.make_async_remote_copy(
        src_ref=every,
        dst_ref=every,
        send_sem=offs_send,
        recv_sem=offs_recv,
        device_id={"shift": t},
        device_id_type=MESH,
    )
    whole.wait_recv()
    whole.wait_send()

    for group, first in enumerate(firsts):
        place = r - first

        @pl.when((place >= 0) & (place <= 2))
        def _():
            def done(k, c):
                block_copy(3, r, send_sem.at[group, k]).wait_send()
                return c

            lax.fori_loop(1, ROWS, done, 0)

    @pl.when(r >= 1)
    def _():
        block_copy(0, r, near_sem.at[0]).wait_send()

    block_copy(1, r, near_sem.at[1]).wait_send()

    @pl.when((r >= 1) & (r != 16))
    def _():
        block_copy(2, r, near_sem.at[2]).wait_send()


def lower_inverse(gram):
    lanes = lax.broadcasted_iota(jnp.int32, (8, 128), 1)
    subs = lax.broadcasted_iota(jnp.int32, (8, 128), 0)
    rows = [gram[8 * i : 8 * i + 8] + jnp.where(lanes == subs + 8 * i, 1.0, 0.0) for i in range(8)]
    out = []
    for b in range(8):
        cols = [
            {i: jnp.broadcast_to(rows[i][:, 64 + 8 * b + j : 65 + 8 * b + j], (8, 128)) for i in range(b, 8)}
            for j in range(8)
        ]
        scale = jnp.zeros((8, 128), F32)
        for j in range(8):
            pivot = jnp.broadcast_to(cols[j][b][j : j + 1], (8, 128))
            root = lax.rsqrt(pivot)
            inverse = root * root
            scale = jnp.where(subs == j, root, scale)
            lead = jnp.broadcast_to(rows[b][j : j + 1], (8, 128))
            heads = {l: jnp.broadcast_to(cols[l][b][j : j + 1], (8, 128)) for l in range(j + 1, 8)}
            for i in range(b, 8):
                factor = cols[j][i] * inverse
                if i == b:
                    factor = jnp.where(subs > j, factor, 0.0)
                rows[i] = rows[i] - factor * lead
                for l in range(j + 1, 8):
                    cols[l][i] = cols[l][i] - factor * heads[l]
        out.append(rows[b] * scale)
    return jnp.concatenate(out, 0)[:, :64]


def padded_gram(x):
    both = jnp.concatenate([jnp.zeros_like(x), x], 0)
    return lax.dot_general(x, both, (((1,), (1,)), ((), ())), precision=HIGHEST, preferred_element_type=F32)


def music_kernel(
    own_ref, got_ref, offs_ref, start_ref, cov_ref, basis_ref,
    row_w, row_m, col_w, col_m, acc,
    part1, land1, map1, part2, land2, sum2, part3, land3, sum3,
    send_sem, recv_sem,
):
    r = lax.axis_index("row")
    t = lax.axis_index("shift")
    barrier = pltpu.get_barrier_semaphore()
    signal_peers(barrier, r, t)

    up = lax.broadcasted_iota(jnp.int32, (BLOCK, BLOCK), 0)
    across = lax.broadcasted_iota(jnp.int32, (BLOCK, BLOCK), 1)
    flip = jnp.where(up + across == BLOCK - 1, 1.0, 0.0).astype(BF16)

    def put(window, place, block, top):
        re, im = block[0].astype(F32) * HALF_ROOT, block[1].astype(F32) * HALF_ROOT
        window[0, pl.ds(place * BLOCK, BLOCK), :] = jnp.where(top, re, im)
        window[1, pl.ds(place * BLOCK, BLOCK), :] = jnp.where(top, im, -re)

    def put_flipped(mirror, place, block, top):
        re = jnp.dot(flip, block[0], preferred_element_type=F32) * HALF_ROOT
        im = jnp.dot(flip, block[1], preferred_element_type=F32) * HALF_ROOT
        mirror[0, pl.ds(place * BLOCK, BLOCK), :] = jnp.where(top, re, -im)
        mirror[1, pl.ds(place * BLOCK, BLOCK), :] = jnp.where(top, im, re)

    row_top, col_top = r < ROWS // 2, t < COLS // 2
    put(row_w, 0, own_ref[...], row_top)
    put(row_w, 1, got_ref[0], row_top)
    put_flipped(row_m, 0, got_ref[2], row_top)
    put_flipped(row_m, 1, got_ref[1], row_top)
    for place in range(3):
        put(col_w, place, got_ref[3 + place], col_top)
        put_flipped(col_m, place, got_ref[8 - place], col_top)

    def pairs(window, mirror, offset, count):
        parts = []
        for c in range(2):
            a = window[c, pl.ds(offset, count), :]
            b = mirror[c, pl.ds(BLOCK - offset, count), :]
            parts.append((a + b).astype(BF16))
        return parts

    acc[...] = jnp.zeros_like(acc)

    def some(i, c):
        lhs, rhs = [], []
        for j in range(3):
            offset = offs_ref[i, 0, j]
            lhs += pairs(row_w, row_m, offset, BLOCK)
            rhs += pairs(col_w, col_m, offset, 2 * BLOCK)
        acc[...] += lax.dot_general(
            jnp.concatenate(lhs, 1), jnp.concatenate(rhs, 1), (((1,), (1,)), ((), ())), preferred_element_type=F32
        )
        return c

    lax.fori_loop(0, COLS, some, 0)
    cov = acc[...] * (1.0 / (SNAPS * SHIFTS))
    cov_ref[...] = cov

    first = jnp.dot(start_ref[...], cov, precision=HIGHEST, preferred_element_type=F32)
    for c in range(2):
        for a in range(8):
            part1[8 * c + a] = first[8 * a : 8 * a + 8, BLOCK * c : BLOCK * c + BLOCK]

    pl.semaphore_wait(barrier, ROWS - 1 + COLS - 1)

    def copy(src, dst, phase, where):
        return pltpu.make_async_remote_copy(
            src_ref=src,
            dst_ref=dst,
            send_sem=send_sem.at[phase],
            recv_sem=recv_sem.at[phase],
            device_id=where,
            device_id_type=MESH,
        )

    def over(count, body):
        def step(k, c):
            body(k)
            return c

        lax.fori_loop(1, count, step, 0)

    def total(phase, buffer, count):
        every = buffer.at[pl.ds(0, count)]
        return copy(every, every, phase, {"row": r})

    def scatter1(k):
        dest = lax.rem(r + k, ROWS)
        copy(part1.at[dest // 2], land1.at[r], 0, {"row": dest}).start()

    over(ROWS, scatter1)
    land1[r] = part1[r // 2]
    total(0, land1, ROWS - 1).wait_recv()
    mine = r // 2
    map1[mine] = jnp.sum(land1[...], axis=0)

    def spread1(k):
        copy(map1.at[mine], map1.at[mine], 1, {"row": lax.rem(r + 2 * k, ROWS)}).start()

    over(ROWS // 2, spread1)
    total(1, map1, ROWS // 2 - 1).wait_recv()
    mapped = jnp.concatenate([map1[0:8].reshape(K, BLOCK), map1[8:16].reshape(K, BLOCK)], 1)

    gram1 = padded_gram(mapped)
    second = lax.dot_general(
        mapped, cov_ref[...], (((1,), (1,)), ((), ())), precision=HIGHEST, preferred_element_type=F32
    )
    for a in range(8):
        part2[a] = second[8 * a : 8 * a + 8]
        part2[8 + a] = gram1[8 * a : 8 * a + 8]

    def scatter2(k):
        dest = lax.rem(t + k, COLS)
        copy(part2.at[dest], land2.at[t], 2, {"shift": dest}).start()

    over(COLS, scatter2)
    land2[t] = part2[t]
    total(2, land2, COLS - 1).wait_recv()
    sum2[t] = jnp.sum(land2[...], axis=0)

    def spread2(k):
        copy(sum2.at[t], sum2.at[t], 3, {"shift": lax.rem(t + k, COLS)}).start()

    over(COLS, spread2)
    total(3, sum2, COLS - 1).wait_recv()
    factor1 = lower_inverse(sum2[8:16].reshape(K, BLOCK))
    mapped2 = jnp.dot(factor1, sum2[0:8].reshape(K, BLOCK), precision=HIGHEST, preferred_element_type=F32)
    gram2 = padded_gram(mapped2)
    for a in range(16):
        part3[a] = gram2[4 * a : 4 * a + 4]

    def spread3(k):
        copy(part3.at[t], land3.at[r], 4, {"row": lax.rem(r + k, ROWS)}).start()

    over(ROWS, spread3)
    land3[r] = part3[t]
    total(4, land3, ROWS - 1).wait_recv()
    sum3[t] = jnp.sum(land3[...], axis=0)

    def spread4(k):
        copy(sum3.at[t], sum3.at[t], 5, {"shift": lax.rem(t + k, COLS)}).start()

    over(COLS, spread4)
    total(5, sum3, COLS - 1).wait_recv()
    whole = jnp.concatenate([sum3[a] for a in range(16)], 0)
    factor2 = lower_inverse(whole)
    basis_ref[...] = jnp.dot(factor2, mapped2, precision=HIGHEST, preferred_element_type=F32)

    total(0, land1, ROWS - 1).wait_send()
    total(1, map1, ROWS // 2 - 1).wait_send()
    total(2, land2, COLS - 1).wait_send()
    total(3, sum2, COLS - 1).wait_send()
    total(4, land3, ROWS - 1).wait_send()
    total(5, sum3, COLS - 1).wait_send()


def per_device(snapshots, tail_sensors, shift_offsets, start_basis):
    own = snapshots.transpose(1, 0, 2)
    tail = tail_sensors.transpose(1, 0, 2)
    offs = jnp.pad(shift_offsets, (0, BLOCK - shift_offsets.shape[0])).reshape(1, BLOCK)
    vmem = pl.BlockSpec(memory_space=pltpu.VMEM)
    smem = pl.BlockSpec(memory_space=pltpu.SMEM)
    dma = pltpu.SemaphoreType.DMA
    got, every_offs = pl.pallas_call(
        gather_kernel,
        out_shape=(
            jax.ShapeDtypeStruct((9, 2, BLOCK, SNAPS), BF16),
            jax.ShapeDtypeStruct((COLS, 1, BLOCK), jnp.int32),
        ),
        in_specs=[vmem] * 3,
        out_specs=(vmem, vmem),
        scratch_shapes=[dma((2, ROWS)), dma((3,)), dma((9,)), dma, dma],
        compiler_params=pltpu.CompilerParams(collective_id=0, has_side_effects=True),
        name="gather_sensors",
    )(own, tail, offs)
    f32 = lambda *shape: pltpu.VMEM(shape, F32)
    return pl.pallas_call(
        music_kernel,
        out_shape=(
            jax.ShapeDtypeStruct((BLOCK, 2 * BLOCK), F32),
            jax.ShapeDtypeStruct((K, BLOCK), F32),
        ),
        in_specs=[vmem, vmem, smem, vmem],
        out_specs=(vmem, vmem),
        scratch_shapes=[
            f32(2, 256, 128), f32(2, 256, 128), f32(2, 384, 128), f32(2, 384, 128), f32(128, 256),
            f32(16, 8, 128), f32(32, 8, 128), f32(16, 8, 128),
            f32(16, 8, 128), f32(16, 8, 128), f32(16, 8, 128),
            f32(16, 4, 128), f32(32, 4, 128), f32(16, 4, 128),
            dma((6,)), dma((6,)),
        ],
        compiler_params=pltpu.CompilerParams(collective_id=1, has_side_effects=True),
        name="music",
    )(own, got, every_offs, start_basis)


def solution(mesh):
    in_specs = (P("row", None, None), P(), P("shift"), P(None, "row"))
    out_specs = (P("row", "shift"), P(None, "row"))
    return jax.shard_map(per_device, mesh=mesh, in_specs=in_specs, out_specs=out_specs, check_vma=False)
```

```python
import jax
import jax.numpy as jnp
from jax import lax
from jax.experimental import pallas as pl
from jax.experimental.pallas import tpu as pltpu
from jax.sharding import PartitionSpec as P

M = 4096
K = 64
SNAPS = 128
SHIFTS = 48
ROWS = 32
COLS = 16
BLOCK = 128
HALF_ROOT = 0.7071067811865476
MESH = pl.DeviceIdType.MESH
HIGHEST = lax.Precision.HIGHEST
F32 = jnp.float32
BF16 = jnp.bfloat16


def signal_peers(barrier, r, t):
    def plane(k, _):
        pl.semaphore_signal(
            barrier, inc=1, device_id={"row": lax.rem(r + k, ROWS)}, device_id_type=MESH
        )
        return _

    def line(k, _):
        pl.semaphore_signal(
            barrier, inc=1, device_id={"shift": lax.rem(t + k, COLS)}, device_id_type=MESH
        )
        return _

    lax.fori_loop(1, ROWS, plane, 0)
    lax.fori_loop(1, COLS, line, 0)


def lower_inverse(gram):
    lanes = lax.broadcasted_iota(jnp.int32, (8, 128), 1)
    subs = lax.broadcasted_iota(jnp.int32, (8, 128), 0)
    rows = [gram[8 * i : 8 * i + 8] + jnp.where(lanes == subs + 8 * i, 1.0, 0.0) for i in range(8)]
    out = []
    for b in range(8):
        cols = [
            {i: jnp.broadcast_to(rows[i][:, 64 + 8 * b + j : 65 + 8 * b + j], (8, 128)) for i in range(b, 8)}
            for j in range(8)
        ]
        scale = jnp.zeros((8, 128), F32)
        for j in range(8):
            pivot = jnp.broadcast_to(cols[j][b][j : j + 1], (8, 128))
            root = lax.rsqrt(pivot)
            inverse = root * root
            scale = jnp.where(subs == j, root, scale)
            lead = jnp.broadcast_to(rows[b][j : j + 1], (8, 128))
            heads = {l: jnp.broadcast_to(cols[l][b][j : j + 1], (8, 128)) for l in range(j + 1, 8)}
            for i in range(b, 8):
                factor = cols[j][i] * inverse
                if i == b:
                    factor = jnp.where(subs > j, factor, 0.0)
                rows[i] = rows[i] - factor * lead
                for l in range(j + 1, 8):
                    cols[l][i] = cols[l][i] - factor * heads[l]
        out.append(rows[b] * scale)
    return jnp.concatenate(out, 0)[:, :64]


def padded_gram(x):
    both = jnp.concatenate([jnp.zeros_like(x), x], 0)
    return lax.dot_general(x, both, (((1,), (1,)), ((), ())), precision=HIGHEST, preferred_element_type=F32)


def selection(top, flipped):
    out = lax.broadcasted_iota(jnp.int32, (2 * BLOCK, 2 * BLOCK), 0)
    src = lax.broadcasted_iota(jnp.int32, (2 * BLOCK, 2 * BLOCK), 1)
    second = out >= BLOCK
    sensor = jnp.where(second, out - BLOCK, out)
    if flipped:
        sensor = BLOCK - 1 - sensor
    straight = jnp.where(second, 2 * sensor + 1, 2 * sensor)
    crossed = jnp.where(second, 2 * sensor, 2 * sensor + 1)
    minus = second if not flipped else jnp.logical_not(second)
    upper = jnp.where(src == straight, 1.0, 0.0)
    lower = jnp.where(src == crossed, jnp.where(minus, -1.0, 1.0), 0.0)
    return jnp.where(top, upper, lower).astype(BF16)


def music_kernel(
    own_ref, tail_ref, offs_ref, start_ref, cov_ref, basis_ref,
    got, picks, offs_all, offs_near, offs_now,
    row_w, row_m, col_w, col_m, acc,
    part1, land1, map1, part2, land2, sum2, part3, land3, sum3,
    wide_send, wide_recv, near_send, near_recv, offs_send, offs_recv, local_sem,
    send_sem, recv_sem,
):
    r = lax.axis_index("row")
    t = lax.axis_index("shift")
    x, y = r // 8, r % 8
    core = t % 2
    barrier = pltpu.get_barrier_semaphore()
    signal_peers(barrier, r, t)

    lane = lax.broadcasted_iota(jnp.int32, (1, BLOCK), 1)
    offs_near[...] = jnp.where(lane == 0, offs_ref[0], jnp.where(lane == 1, offs_ref[1], offs_ref[2]))
    row_top, col_top = r < ROWS // 2, t < COLS // 2
    picks[0] = selection(row_top, False)
    picks[1] = selection(row_top, True)
    picks[2] = selection(col_top, False)
    picks[3] = selection(col_top, True)
    acc[...] = jnp.zeros_like(acc)
    pl.semaphore_wait(barrier, ROWS - 1 + COLS - 1)

    def wide(src, slot, k, dest):
        return pltpu.make_async_remote_copy(
            src_ref=src,
            dst_ref=got.at[slot],
            send_sem=wide_send.at[slot - 3, k],
            recv_sem=wide_recv.at[slot - 3],
            device_id={"row": dest},
            device_id_type=MESH,
        )

    slots = []
    for group, first in enumerate((2 * t, 30 - 2 * t)):
        for place in range(3):
            block = first + place
            inside = block < ROWS
            bx, by = block // 8, block % 8
            source = block == r
            column = inside & (x == bx) & (y != by)
            opposite = inside & (x == (bx + 2) % 4) & (y == by)
            slots.append((3 + 3 * group + place, block, source, column, opposite))

    def along_y(src, slot):
        def step(i, c):
            far = 4 + ((i + 1) // 2) * (1 - 2 * (i % 2))
            wide(src, slot, i, x * 8 + (y + far) % 8).start()
            return c

        lax.fori_loop(0, 7, step, 0)

    def along_x(src, slot):
        wide(src, slot, 8, ((x + 1) % 4) * 8 + y).start()
        wide(src, slot, 9, ((x + 3) % 4) * 8 + y).start()

    for slot, block, source, column, opposite in slots:
        @pl.when(source)
        def _():
            wide(own_ref, slot, 7, ((x + 2) % 4) * 8 + y).start()
            along_y(own_ref, slot)
            along_x(own_ref, slot)

    def offs_copy(k):
        return pltpu.make_async_remote_copy(
            src_ref=offs_near,
            dst_ref=offs_all.at[t],
            send_sem=offs_send,
            recv_sem=offs_recv,
            device_id={"shift": (t + k) % COLS},
            device_id_type=MESH,
        )

    def send_offs(k, c):
        offs_copy(k).start()
        return c

    lax.fori_loop(1, COLS, send_offs, 0)
    offs_all[t] = offs_near[...]

    half = pl.ds(pl.multiple_of(core * BLOCK, BLOCK), BLOCK)
    other = pl.ds(pl.multiple_of((1 - core) * BLOCK, BLOCK), BLOCK)

    def near(slot, dest):
        return pltpu.make_async_remote_copy(
            src_ref=own_ref.at[half],
            dst_ref=got.at[slot, half],
            send_sem=near_send.at[slot, 0],
            recv_sem=near_recv.at[slot, 0],
            device_id={"row": dest},
            device_id_type=MESH,
        )

    def pass_on(slot, part):
        return pltpu.make_async_remote_copy(
            src_ref=got.at[slot, part],
            dst_ref=got.at[slot, part],
            send_sem=near_send.at[slot, 1],
            recv_sem=near_recv.at[slot, 1],
            device_id={"shift": t + 1 - 2 * core},
            device_id_type=MESH,
        )

    sends_near = (r >= 1, None, (r >= 1) & (r != 16))
    gets_near = (r != 31, None, (r != 0) & (r != 16))

    def when(condition, body):
        if condition is None:
            body()
        else:
            pl.when(condition)(body)

    for slot, dest in enumerate((r - 1, 31 - r, 32 - r)):
        when(sends_near[slot], lambda: near(slot, dest).start())

    for slot, block, source, column, opposite in slots:
        @pl.when(source)
        def _():
            got[slot] = own_ref[...]

    def from_tail(slot):
        def body():
            got[slot] = tail_ref[...]

        return body

    pl.when(r == 31)(from_tail(0))
    pl.when(r == 0)(from_tail(2))
    pl.when(t == 15)(from_tail(5))
    pl.when(t == 0)(from_tail(8))

    @pl.when(r == 16)
    def _():
        got[2] = own_ref[...]

    def put(window, pick, place, block):
        both = jnp.dot(picks[pick], block, preferred_element_type=F32) * HALF_ROOT
        window[0, pl.ds(place * BLOCK, BLOCK), :] = both[:BLOCK]
        window[1, pl.ds(place * BLOCK, BLOCK), :] = both[BLOCK:]

    put(row_w, 0, 0, own_ref[...])

    for slot, block, source, column, opposite in slots:
        @pl.when(opposite)
        def _():
            wide(own_ref, slot, 0, r).wait_recv()
            along_y(got.at[slot], slot)

    for slot, block, source, column, opposite in slots:
        @pl.when(column)
        def _():
            wide(own_ref, slot, 0, r).wait_recv()
            along_x(got.at[slot], slot)

    for slot in range(3):
        def body():
            near(slot, r).wait_recv()
            pass_on(slot, half).start()

        when(gets_near[slot], body)

    every_offs = offs_all.at[pl.ds(0, COLS - 1)]
    whole_offs = pltpu.make_async_remote_copy(
        src_ref=every_offs,
        dst_ref=every_offs,
        send_sem=offs_send,
        recv_sem=offs_recv,
        device_id={"row": r},
        device_id_type=MESH,
    )
    whole_offs.wait_recv()
    to_scalar = pltpu.make_async_copy(offs_all, offs_now, local_sem)
    to_scalar.start()

    for slot in range(3):
        when(gets_near[slot], lambda: pass_on(slot, other).wait_recv())
    put(row_w, 0, 1, got[0])
    put(row_m, 1, 0, got[2])
    put(row_m, 1, 1, got[1])

    for slot, block, source, column, opposite in slots:
        waits = (block < ROWS) & jnp.logical_not(source | column | opposite)
        pl.when(waits)(lambda: wide(own_ref, slot, 0, r).wait_recv())
    for place in range(3):
        put(col_w, 2, place, got[3 + place])
        put(col_m, 3, place, got[8 - place])
    to_scalar.wait()

    def pairs(window, mirror, offset, count):
        parts = []
        for c in range(2):
            a = window[c, pl.ds(offset, count), :]
            b = mirror[c, pl.ds(BLOCK - offset, count), :]
            parts.append((a + b).astype(BF16))
        return parts

    def some(i, c):
        lhs, rhs = [], []
        for j in range(3):
            offset = offs_now[i, 0, j]
            lhs += pairs(row_w, row_m, offset, BLOCK)
            rhs += pairs(col_w, col_m, offset, 2 * BLOCK)
        acc[...] += lax.dot_general(
            jnp.concatenate(lhs, 1), jnp.concatenate(rhs, 1), (((1,), (1,)), ((), ())), preferred_element_type=F32
        )
        return c

    lax.fori_loop(0, COLS, some, 0)
    cov = acc[...] * (1.0 / (SNAPS * SHIFTS))
    cov_ref[...] = cov

    first = jnp.dot(start_ref[...], cov, precision=HIGHEST, preferred_element_type=F32)
    for c in range(2):
        for a in range(16):
            part1[16 * c + a] = first[4 * a : 4 * a + 4, BLOCK * c : BLOCK * c + BLOCK]

    def copy(src, dst, phase, where):
        return pltpu.make_async_remote_copy(
            src_ref=src,
            dst_ref=dst,
            send_sem=send_sem.at[phase],
            recv_sem=recv_sem.at[phase],
            device_id=where,
            device_id_type=MESH,
        )

    def over(count, body):
        def step(k, c):
            body(k)
            return c

        lax.fori_loop(1, count, step, 0)

    def total(phase, buffer, count):
        every = buffer.at[pl.ds(0, count)]
        return copy(every, every, phase, {"row": r})

    def scatter1(k):
        dest = lax.rem(r + k, ROWS)
        copy(part1.at[dest], land1.at[r], 0, {"row": dest}).start()

    over(ROWS, scatter1)
    land1[r] = part1[r]
    total(0, land1, ROWS - 1).wait_recv()
    map1[r] = jnp.sum(land1[...], axis=0)

    def spread1(k):
        copy(map1.at[r], map1.at[r], 1, {"row": (r + k) % ROWS}).start()

    over(ROWS, spread1)
    total(1, map1, ROWS - 1).wait_recv()
    mapped = jnp.concatenate(
        [jnp.concatenate([map1[16 * c + a] for a in range(16)], 0) for c in range(2)], 1
    )

    gram1 = padded_gram(mapped)
    second = lax.dot_general(
        mapped, cov_ref[...], (((1,), (1,)), ((), ())), precision=HIGHEST, preferred_element_type=F32
    )
    for a in range(8):
        part2[a] = second[8 * a : 8 * a + 8]
        part2[8 + a] = gram1[8 * a : 8 * a + 8]

    def scatter2(k):
        dest = lax.rem(t + k, COLS)
        copy(part2.at[dest], land2.at[t], 2, {"shift": dest}).start()

    over(COLS, scatter2)
    land2[t] = part2[t]
    total(2, land2, COLS - 1).wait_recv()
    sum2[t] = jnp.sum(land2[...], axis=0)

    def spread2(k):
        copy(sum2.at[t], sum2.at[t], 3, {"shift": lax.rem(t + k, COLS)}).start()

    over(COLS, spread2)
    total(3, sum2, COLS - 1).wait_recv()
    factor1 = lower_inverse(sum2[8:16].reshape(K, BLOCK))
    mapped2 = jnp.dot(factor1, sum2[0:8].reshape(K, BLOCK), precision=HIGHEST, preferred_element_type=F32)
    gram2 = padded_gram(mapped2)
    for a in range(16):
        part3[a] = gram2[4 * a : 4 * a + 4]

    def spread3(k):
        copy(part3.at[t], land3.at[r], 4, {"row": lax.rem(r + k, ROWS)}).start()

    over(ROWS, spread3)
    land3[r] = part3[t]
    total(4, land3, ROWS - 1).wait_recv()
    sum3[t] = jnp.sum(land3[...], axis=0)

    def spread4(k):
        copy(sum3.at[t], sum3.at[t], 5, {"shift": lax.rem(t + k, COLS)}).start()

    over(COLS, spread4)
    total(5, sum3, COLS - 1).wait_recv()
    whole = jnp.concatenate([sum3[a] for a in range(16)], 0)
    factor2 = lower_inverse(whole)
    basis_ref[...] = jnp.dot(factor2, mapped2, precision=HIGHEST, preferred_element_type=F32)

    for slot, block, source, column, opposite in slots:
        def drain(low, high):
            def done(k, c):
                wide(own_ref, slot, k, r).wait_send()
                return c

            lax.fori_loop(low, high, done, 0)

        pl.when(source)(lambda: drain(0, 10))
        pl.when(column)(lambda: drain(8, 10))
        pl.when(opposite)(lambda: drain(0, 7))
    for slot in range(3):
        when(sends_near[slot], lambda: near(slot, r).wait_send())
        when(gets_near[slot], lambda: pass_on(slot, half).wait_send())
    whole_offs.wait_send()
    total(0, land1, ROWS - 1).wait_send()
    total(1, map1, ROWS - 1).wait_send()
    total(2, land2, COLS - 1).wait_send()
    total(3, sum2, COLS - 1).wait_send()
    total(4, land3, ROWS - 1).wait_send()
    total(5, sum3, COLS - 1).wait_send()


def per_device(snapshots, tail_sensors, shift_offsets, start_basis):
    own = snapshots.reshape(2 * BLOCK, SNAPS)
    tail = tail_sensors.reshape(2 * BLOCK, SNAPS)
    vmem = pl.BlockSpec(memory_space=pltpu.VMEM)
    smem = pl.BlockSpec(memory_space=pltpu.SMEM)
    dma = pltpu.SemaphoreType.DMA
    f32 = lambda *shape: pltpu.VMEM(shape, F32)
    return pl.pallas_call(
        music_kernel,
        out_shape=(
            jax.ShapeDtypeStruct((BLOCK, 2 * BLOCK), F32),
            jax.ShapeDtypeStruct((K, BLOCK), F32),
        ),
        in_specs=[vmem, vmem, smem, vmem],
        out_specs=(vmem, vmem),
        scratch_shapes=[
            pltpu.VMEM((9, 256, 128), BF16), pltpu.VMEM((4, 256, 256), BF16),
            pltpu.VMEM((COLS, 1, BLOCK), jnp.int32), pltpu.VMEM((1, BLOCK), jnp.int32),
            pltpu.SMEM((COLS, 1, BLOCK), jnp.int32),
            f32(2, 256, 128), f32(2, 256, 128), f32(2, 384, 128), f32(2, 384, 128), f32(128, 256),
            f32(32, 4, 128), f32(32, 4, 128), f32(32, 4, 128),
            f32(16, 8, 128), f32(16, 8, 128), f32(16, 8, 128),
            f32(16, 4, 128), f32(32, 4, 128), f32(16, 4, 128),
            dma((6, 10)), dma((6,)), dma((3, 2)), dma((3, 2)), dma, dma, dma,
            dma((6,)), dma((6,)),
        ],
        compiler_params=pltpu.CompilerParams(collective_id=0, has_side_effects=True),
        name="music",
    )(own, tail, shift_offsets, start_basis)


def solution(mesh):
    in_specs = (P("row", None, None), P(), P("shift"), P(None, "row"))
    out_specs = (P("row", "shift"), P(None, "row"))
    return jax.shard_map(per_device, mesh=mesh, in_specs=in_specs, out_specs=out_specs, check_vma=False)
```

```python
import jax
import jax.numpy as jnp
from jax import lax
from jax.experimental import pallas as pl
from jax.experimental.pallas import tpu as pltpu
from jax.sharding import PartitionSpec as P

M = 4096
K = 64
SNAPS = 128
SHIFTS = 48
ROWS = 32
COLS = 16
BLOCK = 128
HALF_ROOT = 0.7071067811865476
MESH = pl.DeviceIdType.MESH
HIGHEST = lax.Precision.HIGHEST
F32 = jnp.float32
BF16 = jnp.bfloat16


def signal_peers(barrier, r, t):
    def plane(k, _):
        pl.semaphore_signal(
            barrier, inc=1, device_id={"row": lax.rem(r + k, ROWS)}, device_id_type=MESH
        )
        return _

    def line(k, _):
        pl.semaphore_signal(
            barrier, inc=1, device_id={"shift": lax.rem(t + k, COLS)}, device_id_type=MESH
        )
        return _

    lax.fori_loop(1, ROWS, plane, 0)
    lax.fori_loop(1, COLS, line, 0)


def lower_inverse(gram):
    lanes = lax.broadcasted_iota(jnp.int32, (8, 128), 1)
    subs = lax.broadcasted_iota(jnp.int32, (8, 128), 0)
    rows = [gram[8 * i : 8 * i + 8] + jnp.where(lanes == subs + 8 * i, 1.0, 0.0) for i in range(8)]
    out = []
    for b in range(8):
        cols = [
            {i: jnp.broadcast_to(rows[i][:, 64 + 8 * b + j : 65 + 8 * b + j], (8, 128)) for i in range(b, 8)}
            for j in range(8)
        ]
        scale = jnp.zeros((8, 128), F32)
        for j in range(8):
            pivot = jnp.broadcast_to(cols[j][b][j : j + 1], (8, 128))
            root = lax.rsqrt(pivot)
            inverse = root * root
            scale = jnp.where(subs == j, root, scale)
            lead = jnp.broadcast_to(rows[b][j : j + 1], (8, 128))
            heads = {l: jnp.broadcast_to(cols[l][b][j : j + 1], (8, 128)) for l in range(j + 1, 8)}
            for i in range(b, 8):
                factor = cols[j][i] * inverse
                if i == b:
                    factor = jnp.where(subs > j, factor, 0.0)
                rows[i] = rows[i] - factor * lead
                for l in range(j + 1, 8):
                    cols[l][i] = cols[l][i] - factor * heads[l]
        out.append(rows[b] * scale)
    return jnp.concatenate(out, 0)[:, :64]


def padded_gram(x):
    both = jnp.concatenate([jnp.zeros_like(x), x], 0)
    return lax.dot_general(x, both, (((1,), (1,)), ((), ())), precision=HIGHEST, preferred_element_type=F32)


def selection(top, flipped):
    out = lax.broadcasted_iota(jnp.int32, (2 * BLOCK, 2 * BLOCK), 0)
    src = lax.broadcasted_iota(jnp.int32, (2 * BLOCK, 2 * BLOCK), 1)
    second = out >= BLOCK
    sensor = jnp.where(second, out - BLOCK, out)
    if flipped:
        sensor = BLOCK - 1 - sensor
    straight = jnp.where(second, 2 * sensor + 1, 2 * sensor)
    crossed = jnp.where(second, 2 * sensor, 2 * sensor + 1)
    minus = second if not flipped else jnp.logical_not(second)
    upper = jnp.where(src == straight, 1.0, 0.0)
    lower = jnp.where(src == crossed, jnp.where(minus, -1.0, 1.0), 0.0)
    return jnp.where(top, upper, lower).astype(BF16)


def music_kernel(
    own_ref, tail_ref, offs_ref, start_ref, cov_ref, basis_ref,
    got, picks, offs_all, offs_near, offs_now,
    row_w, row_m, col_w, col_m, acc,
    part1, land1, map1, part2, land2, sum2, part3, land3, sum3,
    wide_send, wide_recv, near_send, near_recv, offs_send, offs_recv, local_sem,
    send_sem, recv_sem,
):
    r = lax.axis_index("row")
    t = lax.axis_index("shift")
    x, y = r // 8, r % 8
    core = t % 2
    barrier = pltpu.get_barrier_semaphore()
    signal_peers(barrier, r, t)

    lane = lax.broadcasted_iota(jnp.int32, (1, BLOCK), 1)
    offs_near[...] = jnp.where(lane == 0, offs_ref[0], jnp.where(lane == 1, offs_ref[1], offs_ref[2]))
    row_top, col_top = r < ROWS // 2, t < COLS // 2
    picks[0] = selection(row_top, False)
    picks[1] = selection(row_top, True)
    picks[2] = selection(col_top, False)
    picks[3] = selection(col_top, True)
    acc[...] = jnp.zeros_like(acc)
    pl.semaphore_wait(barrier, ROWS - 1 + COLS - 1)

    def wide(src, slot, k, dest):
        return pltpu.make_async_remote_copy(
            src_ref=src,
            dst_ref=got.at[slot],
            send_sem=wide_send.at[slot - 3, k],
            recv_sem=wide_recv.at[slot - 3],
            device_id={"row": dest},
            device_id_type=MESH,
        )

    slots = []
    for group, first in enumerate((2 * t, 30 - 2 * t)):
        for place in range(3):
            block = first + place
            inside = block < ROWS
            bx, by = block // 8, block % 8
            source = block == r
            column = inside & (x == bx) & (y != by)
            opposite = inside & (x == (bx + 2) % 4) & (y == by)
            slots.append((3 + 3 * group + place, block, source, column, opposite))

    def along_y(src, slot):
        def step(i, c):
            far = 4 + ((i + 1) // 2) * (1 - 2 * (i % 2))
            wide(src, slot, i, x * 8 + (y + far) % 8).start()
            return c

        lax.fori_loop(0, 7, step, 0)

    def along_x(src, slot):
        wide(src, slot, 8, ((x + 1) % 4) * 8 + y).start()
        wide(src, slot, 9, ((x + 3) % 4) * 8 + y).start()

    for slot, block, source, column, opposite in slots:
        @pl.when(source)
        def _():
            wide(own_ref, slot, 7, ((x + 2) % 4) * 8 + y).start()
            along_y(own_ref, slot)
            along_x(own_ref, slot)

    def offs_copy(k):
        return pltpu.make_async_remote_copy(
            src_ref=offs_near,
            dst_ref=offs_all.at[t],
            send_sem=offs_send,
            recv_sem=offs_recv,
            device_id={"shift": (t + k) % COLS},
            device_id_type=MESH,
        )

    def send_offs(k, c):
        offs_copy(k).start()
        return c

    lax.fori_loop(1, COLS, send_offs, 0)
    offs_all[t] = offs_near[...]

    half = pl.ds(pl.multiple_of(core * BLOCK, BLOCK), BLOCK)
    other = pl.ds(pl.multiple_of((1 - core) * BLOCK, BLOCK), BLOCK)

    def near(slot, dest):
        return pltpu.make_async_remote_copy(
            src_ref=own_ref.at[half],
            dst_ref=got.at[slot, half],
            send_sem=near_send.at[slot, 0],
            recv_sem=near_recv.at[slot, 0],
            device_id={"row": dest},
            device_id_type=MESH,
        )

    def pass_on(slot, part):
        return pltpu.make_async_remote_copy(
            src_ref=got.at[slot, part],
            dst_ref=got.at[slot, part],
            send_sem=near_send.at[slot, 1],
            recv_sem=near_recv.at[slot, 1],
            device_id={"shift": t + 1 - 2 * core},
            device_id_type=MESH,
        )

    sends_near = (r >= 1, None, (r >= 1) & (r != 16))
    gets_near = (r != 31, None, (r != 0) & (r != 16))

    def when(condition, body):
        if condition is None:
            body()
        else:
            pl.when(condition)(body)

    for slot, dest in enumerate((r - 1, 31 - r, 32 - r)):
        when(sends_near[slot], lambda: near(slot, dest).start())

    for slot, block, source, column, opposite in slots:
        @pl.when(source)
        def _():
            got[slot] = own_ref[...]

    def from_tail(slot):
        def body():
            got[slot] = tail_ref[...]

        return body

    pl.when(r == 31)(from_tail(0))
    pl.when(r == 0)(from_tail(2))
    pl.when(t == 15)(from_tail(5))
    pl.when(t == 0)(from_tail(8))

    @pl.when(r == 16)
    def _():
        got[2] = own_ref[...]

    def put(window, pick, place, block):
        both = jnp.dot(picks[pick], block, preferred_element_type=F32) * HALF_ROOT
        window[0, pl.ds(place * BLOCK, BLOCK), :] = both[:BLOCK]
        window[1, pl.ds(place * BLOCK, BLOCK), :] = both[BLOCK:]

    put(row_w, 0, 0, own_ref[...])

    for slot, block, source, column, opposite in slots:
        @pl.when(opposite)
        def _():
            wide(own_ref, slot, 0, r).wait_recv()
            along_y(got.at[slot], slot)

    for slot, block, source, column, opposite in slots:
        @pl.when(column)
        def _():
            wide(own_ref, slot, 0, r).wait_recv()
            along_x(got.at[slot], slot)

    for slot in range(3):
        def body():
            near(slot, r).wait_recv()
            pass_on(slot, half).start()

        when(gets_near[slot], body)

    every_offs = offs_all.at[pl.ds(0, COLS - 1)]
    whole_offs = pltpu.make_async_remote_copy(
        src_ref=every_offs,
        dst_ref=every_offs,
        send_sem=offs_send,
        recv_sem=offs_recv,
        device_id={"row": r},
        device_id_type=MESH,
    )
    whole_offs.wait_recv()
    to_scalar = pltpu.make_async_copy(offs_all, offs_now, local_sem)
    to_scalar.start()

    for slot in range(3):
        when(gets_near[slot], lambda: pass_on(slot, other).wait_recv())
    put(row_w, 0, 1, got[0])
    put(row_m, 1, 0, got[2])
    put(row_m, 1, 1, got[1])

    for slot, block, source, column, opposite in slots:
        waits = (block < ROWS) & jnp.logical_not(source | column | opposite)
        pl.when(waits)(lambda: wide(own_ref, slot, 0, r).wait_recv())
    for place in range(3):
        put(col_w, 2, place, got[3 + place])
        put(col_m, 3, place, got[8 - place])
    to_scalar.wait()

    def pairs(window, mirror, offset, count):
        parts = []
        for c in range(2):
            a = window[c, pl.ds(offset, count), :]
            b = mirror[c, pl.ds(BLOCK - offset, count), :]
            parts.append((a + b).astype(BF16))
        return parts

    def some(i, c):
        lhs, rhs = [], []
        for j in range(12):
            offset = offs_now[i * 4 + j // 3, 0, j % 3]
            lhs += pairs(row_w, row_m, offset, BLOCK)
            rhs += pairs(col_w, col_m, offset, 2 * BLOCK)
        acc[...] += lax.dot_general(
            jnp.concatenate(lhs, 1), jnp.concatenate(rhs, 1), (((1,), (1,)), ((), ())), preferred_element_type=F32
        )
        return c

    lax.fori_loop(0, 4, some, 0)
    cov = acc[...] * (1.0 / (SNAPS * SHIFTS))
    cov_ref[...] = cov

    first = jnp.dot(start_ref[...], cov, precision=HIGHEST, preferred_element_type=F32)
    for c in range(2):
        for a in range(16):
            part1[16 * c + a] = first[4 * a : 4 * a + 4, BLOCK * c : BLOCK * c + BLOCK]

    def copy(src, dst, phase, where):
        return pltpu.make_async_remote_copy(
            src_ref=src,
            dst_ref=dst,
            send_sem=send_sem.at[phase],
            recv_sem=recv_sem.at[phase],
            device_id=where,
            device_id_type=MESH,
        )

    def over(count, body):
        def step(k, c):
            body(k)
            return c

        lax.fori_loop(1, count, step, 0)

    def total(phase, buffer, count):
        every = buffer.at[pl.ds(0, count)]
        return copy(every, every, phase, {"row": r})

    def scatter1(k):
        dest = lax.rem(r + k, ROWS)
        copy(part1.at[dest], land1.at[r], 0, {"row": dest}).start()

    over(ROWS, scatter1)
    land1[r] = part1[r]
    total(0, land1, ROWS - 1).wait_recv()
    map1[r] = jnp.sum(land1[...], axis=0)

    def spread1(k):
        copy(map1.at[r], map1.at[r], 1, {"row": (r + k) % ROWS}).start()

    over(ROWS, spread1)
    total(1, map1, ROWS - 1).wait_recv()
    mapped = jnp.concatenate(
        [jnp.concatenate([map1[16 * c + a] for a in range(16)], 0) for c in range(2)], 1
    )

    gram1 = padded_gram(mapped)
    second = lax.dot_general(
        mapped, cov_ref[...], (((1,), (1,)), ((), ())), precision=HIGHEST, preferred_element_type=F32
    )
    for a in range(8):
        part2[a] = second[8 * a : 8 * a + 8]
        part2[8 + a] = gram1[8 * a : 8 * a + 8]

    def scatter2(k):
        dest = lax.rem(t + k, COLS)
        copy(part2.at[dest], land2.at[t], 2, {"shift": dest}).start()

    over(COLS, scatter2)
    land2[t] = part2[t]
    total(2, land2, COLS - 1).wait_recv()
    sum2[t] = jnp.sum(land2[...], axis=0)

    def spread2(k):
        copy(sum2.at[t], sum2.at[t], 3, {"shift": lax.rem(t + k, COLS)}).start()

    over(COLS, spread2)
    total(3, sum2, COLS - 1).wait_recv()
    factor1 = lower_inverse(sum2[8:16].reshape(K, BLOCK))
    mapped2 = jnp.dot(factor1, sum2[0:8].reshape(K, BLOCK), precision=HIGHEST, preferred_element_type=F32)
    gram2 = padded_gram(mapped2)
    for a in range(16):
        part3[a] = gram2[4 * a : 4 * a + 4]

    def spread3(k):
        copy(part3.at[t], land3.at[r], 4, {"row": lax.rem(r + k, ROWS)}).start()

    over(ROWS, spread3)
    land3[r] = part3[t]
    total(4, land3, ROWS - 1).wait_recv()
    sum3[t] = jnp.sum(land3[...], axis=0)

    def spread4(k):
        copy(sum3.at[t], sum3.at[t], 5, {"shift": lax.rem(t + k, COLS)}).start()

    over(COLS, spread4)
    total(5, sum3, COLS - 1).wait_recv()
    whole = jnp.concatenate([sum3[a] for a in range(16)], 0)
    factor2 = lower_inverse(whole)
    basis_ref[...] = jnp.dot(factor2, mapped2, precision=HIGHEST, preferred_element_type=F32)

    for slot, block, source, column, opposite in slots:
        def drain(low, high):
            def done(k, c):
                wide(own_ref, slot, k, r).wait_send()
                return c

            lax.fori_loop(low, high, done, 0)

        pl.when(source)(lambda: drain(0, 10))
        pl.when(column)(lambda: drain(8, 10))
        pl.when(opposite)(lambda: drain(0, 7))
    for slot in range(3):
        when(sends_near[slot], lambda: near(slot, r).wait_send())
        when(gets_near[slot], lambda: pass_on(slot, half).wait_send())
    whole_offs.wait_send()
    total(0, land1, ROWS - 1).wait_send()
    total(1, map1, ROWS - 1).wait_send()
    total(2, land2, COLS - 1).wait_send()
    total(3, sum2, COLS - 1).wait_send()
    total(4, land3, ROWS - 1).wait_send()
    total(5, sum3, COLS - 1).wait_send()


def per_device(snapshots, tail_sensors, shift_offsets, start_basis):
    own = snapshots.reshape(2 * BLOCK, SNAPS)
    tail = tail_sensors.reshape(2 * BLOCK, SNAPS)
    vmem = pl.BlockSpec(memory_space=pltpu.VMEM)
    smem = pl.BlockSpec(memory_space=pltpu.SMEM)
    dma = pltpu.SemaphoreType.DMA
    f32 = lambda *shape: pltpu.VMEM(shape, F32)
    return pl.pallas_call(
        music_kernel,
        out_shape=(
            pltpu.VMEM((BLOCK, 2 * BLOCK), F32),
            pltpu.VMEM((K, BLOCK), F32),
        ),
        in_specs=[vmem, vmem, smem, vmem],
        out_specs=(vmem, vmem),
        scratch_shapes=[
            pltpu.VMEM((9, 256, 128), BF16), pltpu.VMEM((4, 256, 256), BF16),
            pltpu.VMEM((COLS, 1, BLOCK), jnp.int32), pltpu.VMEM((1, BLOCK), jnp.int32),
            pltpu.SMEM((COLS, 1, BLOCK), jnp.int32),
            f32(2, 256, 128), f32(2, 256, 128), f32(2, 384, 128), f32(2, 384, 128), f32(128, 256),
            f32(32, 4, 128), f32(32, 4, 128), f32(32, 4, 128),
            f32(16, 8, 128), f32(16, 8, 128), f32(16, 8, 128),
            f32(16, 4, 128), f32(32, 4, 128), f32(16, 4, 128),
            dma((6, 10)), dma((6,)), dma((3, 2)), dma((3, 2)), dma, dma, dma,
            dma((6,)), dma((6,)),
        ],
        compiler_params=pltpu.CompilerParams(collective_id=0, has_side_effects=True),
        name="music",
    )(own, tail, shift_offsets, start_basis)


def solution(mesh):
    in_specs = (P("row", None, None), P(), P("shift"), P(None, "row"))
    out_specs = (P("row", "shift"), P(None, "row"))
    return jax.shard_map(per_device, mesh=mesh, in_specs=in_specs, out_specs=out_specs, check_vma=False)
```

```python
import jax
import jax.numpy as jnp
from jax import lax
from jax.experimental import pallas as pl
from jax.experimental.pallas import tpu as pltpu
from jax.sharding import PartitionSpec as P

M = 4096
K = 64
SNAPS = 128
SHIFTS = 48
ROWS = 32
COLS = 16
BLOCK = 128
HALF_ROOT = 0.7071067811865476
MESH = pl.DeviceIdType.MESH
HIGHEST = lax.Precision.HIGHEST
F32 = jnp.float32
BF16 = jnp.bfloat16


def far_first(n):
    return sorted(range(n), key=lambda d: -min(d, n - d))


def plane_peers(r):
    x, y = lax.div(r, 8), lax.rem(r, 8)
    xs = [lax.rem(x + a, 4) * 8 for a in range(4)]
    ys = [lax.rem(y + b, 8) for b in range(8)]
    order = sorted(
        ((a, b) for a in range(4) for b in range(8) if a or b),
        key=lambda d: -min(d[0], 4 - d[0]) - min(d[1], 8 - d[1]),
    )
    return [xs[a] + ys[b] for a, b in order]


def line_peers(t):
    z, core = lax.div(t, 2), lax.rem(t, 2)
    zs = [lax.rem(z + a, 8) * 2 for a in range(8)]
    cores = [core, 1 - core]
    return [zs[a] + cores[b] for a in far_first(8) for b in (1, 0) if a or b]


def signal_peers(barrier, rows, places):
    for dest in rows:
        pl.semaphore_signal(barrier, inc=1, device_id={"row": dest}, device_id_type=MESH)
    for dest in places:
        pl.semaphore_signal(barrier, inc=1, device_id={"shift": dest}, device_id_type=MESH)


def lower_inverse(gram):
    lanes = lax.broadcasted_iota(jnp.int32, (8, 128), 1)
    subs = lax.broadcasted_iota(jnp.int32, (8, 128), 0)
    rows = [gram[8 * i : 8 * i + 8] + jnp.where(lanes == subs + 8 * i, 1.0, 0.0) for i in range(8)]
    out = []
    for b in range(8):
        cols = [
            {i: jnp.broadcast_to(rows[i][:, 64 + 8 * b + j : 65 + 8 * b + j], (8, 128)) for i in range(b, 8)}
            for j in range(8)
        ]
        scale = jnp.zeros((8, 128), F32)
        for l in range(8):
            cols[l][b] = jnp.where(lanes < 128 + subs, cols[l][b], 0.0)
        for j in range(8):
            root = jnp.broadcast_to(lax.rsqrt(cols[j][b])[j : j + 1], (8, 128))
            inverse = root * root
            scale = jnp.where(subs == j, root, scale)
            lead = jnp.broadcast_to(rows[b][j : j + 1], (8, 128))
            heads = {l: jnp.broadcast_to(cols[l][b][j : j + 1], (8, 128)) for l in range(j + 1, 8)}
            below = jnp.where(subs > j, cols[j][b], 0.0)
            for l in range(j + 1, 8):
                cols[l][b] = cols[l][b] - (below * heads[l]) * inverse
            rows[b] = rows[b] - (below * lead) * inverse
            for i in range(b + 1, 8):
                factor = cols[j][i] * inverse
                rows[i] = rows[i] - factor * lead
                for l in range(j + 1, 8):
                    cols[l][i] = cols[l][i] - factor * heads[l]
        out.append(rows[b] * scale)
    return jnp.concatenate(out, 0)[:, :64]


def padded_gram(x):
    both = jnp.concatenate([jnp.zeros_like(x), x], 0)
    return lax.dot_general(x, both, (((1,), (1,)), ((), ())), precision=HIGHEST, preferred_element_type=F32)


def selection(top, flipped):
    out = lax.broadcasted_iota(jnp.int32, (2 * BLOCK, 2 * BLOCK), 0)
    src = lax.broadcasted_iota(jnp.int32, (2 * BLOCK, 2 * BLOCK), 1)
    second = out >= BLOCK
    sensor = jnp.where(second, out - BLOCK, out)
    if flipped:
        sensor = BLOCK - 1 - sensor
    straight = jnp.where(second, 2 * sensor + 1, 2 * sensor)
    crossed = jnp.where(second, 2 * sensor, 2 * sensor + 1)
    minus = second if not flipped else jnp.logical_not(second)
    upper = jnp.where(src == straight, 1.0, 0.0)
    lower = jnp.where(src == crossed, jnp.where(minus, -1.0, 1.0), 0.0)
    return jnp.where(top, upper, lower).astype(BF16)


def music_kernel(
    own_any, tail_any, offs_ref, start_any, cov_ref, basis_ref,
    own_ref, tail_ref, start_ref,
    got, picks, offs_all, offs_near, offs_now,
    row_w, row_m, col_w, col_m, acc,
    part1, land1, map1, part2, land2, sum2, part3, land3, sum3,
    wide_send, wide_recv, pair_send, pair_recv, near_send, near_recv, offs_send, offs_recv, local_sem,
    send_sem, recv_sem,
):
    r = lax.axis_index("row")
    t = lax.axis_index("shift")
    x, y = lax.div(r, 8), lax.rem(r, 8)
    z, core = lax.div(t, 2), lax.rem(t, 2)
    rows, places = plane_peers(r), line_peers(t)
    column_rows = [x * 8 + lax.rem(y + b, 8) for b in far_first(8) if b]
    bring_own = pltpu.make_async_copy(own_any, own_ref, local_sem.at[1])
    bring_own.start()
    barrier = pltpu.get_barrier_semaphore()
    signal_peers(barrier, rows, places)
    bring_tail = pltpu.make_async_copy(tail_any, tail_ref, local_sem.at[2])
    bring_tail.start()
    bring_start = pltpu.make_async_copy(start_any, start_ref, local_sem.at[3])
    bring_start.start()

    lane = lax.broadcasted_iota(jnp.int32, (1, BLOCK), 1)
    offs_near[...] = jnp.where(lane == 0, offs_ref[0], jnp.where(lane == 1, offs_ref[1], offs_ref[2]))
    half = pl.ds(pl.multiple_of(core * BLOCK, BLOCK), BLOCK)
    other = pl.ds(pl.multiple_of((1 - core) * BLOCK, BLOCK), BLOCK)
    piece = pl.ds(pl.multiple_of(t * 16, 16), 16)
    bring_own.wait()
    pl.semaphore_wait(barrier, ROWS - 1 + COLS - 1)

    slots = []
    for group in range(2):
        if group == 0:
            blocks = (4 * z + 2, 2 * t + 1, 4 * z + 4 * core)
        else:
            blocks = (30 - 4 * z, 31 - 2 * t, 32 - 4 * z - 4 * core)
        for place, block in enumerate(blocks):
            inside = block < ROWS
            bx, by = lax.div(block, 8), lax.rem(block, 8)
            source = block == r
            column = inside & (x == bx) & (y != by)
            opposite = inside & (x == lax.rem(bx + 2, 4)) & (y == by)
            slots.append((3 + 3 * group + place, block, source, column, opposite))

    def shared(slot):
        return slot % 3 == 0

    def wide(slot, k, dest, from_own=False):
        src, dst = own_ref if from_own else got.at[slot], got.at[slot]
        if shared(slot):
            src, dst = src.at[half], dst.at[half]
        return pltpu.make_async_remote_copy(
            src_ref=src,
            dst_ref=dst,
            send_sem=wide_send.at[slot - 3, k],
            recv_sem=wide_recv.at[slot - 3],
            device_id={"row": dest},
            device_id_type=MESH,
        )

    def pair(slot, part):
        return pltpu.make_async_remote_copy(
            src_ref=got.at[slot, part],
            dst_ref=got.at[slot, part],
            send_sem=pair_send.at[slot // 3 - 1],
            recv_sem=pair_recv.at[slot // 3 - 1],
            device_id={"shift": t + 1 - 2 * core},
            device_id_type=MESH,
        )

    def along_y(slot, from_own=False):
        for i, dest in enumerate(column_rows):
            wide(slot, i, dest, from_own).start()

    def along_x(slot, from_own=False):
        wide(slot, 8, lax.rem(x + 1, 4) * 8 + y, from_own).start()
        wide(slot, 9, lax.rem(x + 3, 4) * 8 + y, from_own).start()

    for slot, block, source, column, opposite in slots:
        @pl.when(source)
        def _():
            wide(slot, 7, lax.rem(x + 2, 4) * 8 + y, True).start()
            along_y(slot, True)
            along_x(slot, True)

    def near(slot, dest):
        return pltpu.make_async_remote_copy(
            src_ref=own_ref.at[piece],
            dst_ref=got.at[slot, piece],
            send_sem=near_send.at[slot, 0],
            recv_sem=near_recv.at[slot, 0],
            device_id={"row": dest},
            device_id_type=MESH,
        )

    def pass_on(slot, part, dest):
        return pltpu.make_async_remote_copy(
            src_ref=got.at[slot, part],
            dst_ref=got.at[slot, part],
            send_sem=near_send.at[slot, 1],
            recv_sem=near_recv.at[slot, 1],
            device_id={"shift": dest},
            device_id_type=MESH,
        )

    sends_near = (r >= 1, None, (r >= 1) & (r != 16))
    gets_near = (r != 31, None, (r != 0) & (r != 16))

    def when(condition, body):
        if condition is None:
            body()
        else:
            pl.when(condition)(body)

    for slot, dest in enumerate((r - 1, 31 - r, 32 - r)):
        when(sends_near[slot], lambda: near(slot, dest).start())

    def offs_copy(dest):
        return pltpu.make_async_remote_copy(
            src_ref=offs_near,
            dst_ref=offs_all.at[t],
            send_sem=offs_send,
            recv_sem=offs_recv,
            device_id={"shift": dest},
            device_id_type=MESH,
        )

    for dest in places:
        offs_copy(dest).start()
    offs_all[t] = offs_near[...]

    for slot, block, source, column, opposite in slots:
        @pl.when(opposite)
        def _():
            wide(slot, 0, r).wait_recv()
            along_y(slot)

    for slot in range(3):
        def body():
            near(slot, r).wait_recv()

            for dest in places:
                pass_on(slot, piece, dest).start()

        when(gets_near[slot], body)

    for slot, block, source, column, opposite in slots:
        @pl.when(column)
        def _():
            wide(slot, 0, r).wait_recv()
            along_x(slot)

    for slot, block, source, column, opposite in slots:
        if shared(slot):
            waits = jnp.logical_not(source | column | opposite)
            pl.when(waits)(lambda: wide(slot, 0, r).wait_recv())
            pl.when(jnp.logical_not(source))(lambda: pair(slot, half).start())

    picks[0] = selection(r < ROWS // 2, False)
    picks[1] = selection(r < ROWS // 2, True)
    picks[2] = selection(t < COLS // 2, False)
    picks[3] = selection(t < COLS // 2, True)
    acc[...] = jnp.zeros_like(acc)
    bring_tail.wait()
    bring_start.wait()

    for slot, block, source, column, opposite in slots:
        @pl.when(source)
        def _():
            got[slot] = own_ref[...]

    def from_tail(slot):
        def body():
            got[slot] = tail_ref[...]

        return body

    pl.when(r == 31)(from_tail(0))
    pl.when(r == 0)(from_tail(2))
    pl.when(t == 15)(from_tail(5))
    pl.when(t == 0)(from_tail(8))

    @pl.when(r == 16)
    def _():
        got[2] = own_ref[...]

    def put(window, pick, place, block):
        both = jnp.dot(picks[pick], block, preferred_element_type=F32) * HALF_ROOT
        window[0, pl.ds(place * BLOCK, BLOCK), :] = both[:BLOCK]
        window[1, pl.ds(place * BLOCK, BLOCK), :] = both[BLOCK:]

    put(row_w, 0, 0, own_ref[...])

    every_offs = offs_all.at[pl.ds(0, COLS - 1)]
    whole_offs = pltpu.make_async_remote_copy(
        src_ref=every_offs,
        dst_ref=every_offs,
        send_sem=offs_send,
        recv_sem=offs_recv,
        device_id={"row": r},
        device_id_type=MESH,
    )
    whole_offs.wait_recv()
    to_scalar = pltpu.make_async_copy(offs_all, offs_now, local_sem.at[0])
    to_scalar.start()

    many = pl.ds(0, 16 * (COLS - 1))
    for slot in range(3):
        when(gets_near[slot], lambda: pass_on(slot, many, t).wait_recv())
    put(row_w, 0, 1, got[0])
    put(row_m, 1, 0, got[2])
    put(row_m, 1, 1, got[1])

    for slot, block, source, column, opposite in slots:
        if not shared(slot):
            waits = (block < ROWS) & jnp.logical_not(source | column | opposite)
            pl.when(waits)(lambda: wide(slot, 0, r).wait_recv())
    for slot, block, source, column, opposite in slots:
        if shared(slot):
            pl.when(jnp.logical_not(source))(lambda: pair(slot, other).wait_recv())
    low, high = 2 - 2 * core, 2 * core
    for place, (w, m) in enumerate(((3 + low, 6 + low), (4, 7), (3 + high, 6 + high))):
        put(col_w, 2, place, got[w])
        put(col_m, 3, place, got[m])
    to_scalar.wait()

    def pairs(window, mirror, offset, count):
        parts = []
        for c in range(2):
            a = window[c, pl.ds(offset, count), :]
            b = mirror[c, pl.ds(BLOCK - offset, count), :]
            parts.append((a + b).astype(BF16))
        return parts

    def some(i, c):
        lhs, rhs = [], []
        for j in range(12):
            offset = offs_now[i * 4 + j // 3, 0, j % 3]
            lhs += pairs(row_w, row_m, offset, BLOCK)
            rhs += pairs(col_w, col_m, offset, 2 * BLOCK)
        acc[...] += lax.dot_general(
            jnp.concatenate(lhs, 1), jnp.concatenate(rhs, 1), (((1,), (1,)), ((), ())), preferred_element_type=F32
        )
        return c

    lax.fori_loop(0, 4, some, 0)
    cov = acc[...] * (1.0 / (SNAPS * SHIFTS))
    cov_ref[...] = cov

    first = jnp.dot(start_ref[...], cov, precision=HIGHEST, preferred_element_type=F32)
    for c in range(2):
        for a in range(16):
            part1[16 * c + a] = first[4 * a : 4 * a + 4, BLOCK * c : BLOCK * c + BLOCK]

    def copy(src, dst, phase, where):
        return pltpu.make_async_remote_copy(
            src_ref=src,
            dst_ref=dst,
            send_sem=send_sem.at[phase],
            recv_sem=recv_sem.at[phase],
            device_id=where,
            device_id_type=MESH,
        )

    def total(phase, buffer, count):
        every = buffer.at[pl.ds(0, count)]
        return copy(every, every, phase, {"row": r})

    for dest in rows:
        copy(part1.at[dest], land1.at[r], 0, {"row": dest}).start()
    land1[r] = part1[r]
    total(0, land1, ROWS - 1).wait_recv()
    map1[r] = jnp.sum(land1[...], axis=0)

    for dest in rows:
        copy(map1.at[r], map1.at[r], 1, {"row": dest}).start()
    total(1, map1, ROWS - 1).wait_recv()
    mapped = jnp.concatenate(
        [jnp.concatenate([map1[16 * c + a] for a in range(16)], 0) for c in range(2)], 1
    )

    gram1 = padded_gram(mapped)
    second = lax.dot_general(
        mapped, cov_ref[...], (((1,), (1,)), ((), ())), precision=HIGHEST, preferred_element_type=F32
    )
    for a in range(8):
        part2[a] = second[8 * a : 8 * a + 8]
        part2[8 + a] = gram1[8 * a : 8 * a + 8]

    for dest in places:
        copy(part2.at[dest], land2.at[t], 2, {"shift": dest}).start()
    land2[t] = part2[t]
    total(2, land2, COLS - 1).wait_recv()
    sum2[t] = jnp.sum(land2[...], axis=0)

    for dest in places:
        copy(sum2.at[t], sum2.at[t], 3, {"shift": dest}).start()
    total(3, sum2, COLS - 1).wait_recv()
    factor1 = lower_inverse(sum2[8:16].reshape(K, BLOCK))
    mapped2 = jnp.dot(factor1, sum2[0:8].reshape(K, BLOCK), precision=HIGHEST, preferred_element_type=F32)
    gram2 = padded_gram(mapped2)
    for a in range(16):
        part3[a] = gram2[4 * a : 4 * a + 4]

    for dest in rows:
        copy(part3.at[t], land3.at[r], 4, {"row": dest}).start()
    land3[r] = part3[t]
    total(4, land3, ROWS - 1).wait_recv()
    sum3[t] = jnp.sum(land3[...], axis=0)

    for dest in places:
        copy(sum3.at[t], sum3.at[t], 5, {"shift": dest}).start()
    total(5, sum3, COLS - 1).wait_recv()
    whole = jnp.concatenate([sum3[a] for a in range(16)], 0)
    factor2 = lower_inverse(whole)
    basis_ref[...] = jnp.dot(factor2, mapped2, precision=HIGHEST, preferred_element_type=F32)

    for slot, block, source, column, opposite in slots:
        def drain(low, high):
            def done(k, c):
                wide(slot, k, r).wait_send()
                return c

            lax.fori_loop(low, high, done, 0)

        pl.when(source)(lambda: drain(0, 10))
        pl.when(column)(lambda: drain(8, 10))
        pl.when(opposite)(lambda: drain(0, 7))
        if shared(slot):
            pl.when(jnp.logical_not(source))(lambda: pair(slot, half).wait_send())
    for slot in range(3):
        when(sends_near[slot], lambda: near(slot, r).wait_send())
        when(gets_near[slot], lambda: pass_on(slot, many, t).wait_send())
    whole_offs.wait_send()
    total(0, land1, ROWS - 1).wait_send()
    total(1, map1, ROWS - 1).wait_send()
    total(2, land2, COLS - 1).wait_send()
    total(3, sum2, COLS - 1).wait_send()
    total(4, land3, ROWS - 1).wait_send()
    total(5, sum3, COLS - 1).wait_send()


def per_device(snapshots, tail_sensors, shift_offsets, start_basis):
    own = snapshots.reshape(2 * BLOCK, SNAPS)
    tail = tail_sensors.reshape(2 * BLOCK, SNAPS)
    vmem = pl.BlockSpec(memory_space=pltpu.VMEM)
    smem = pl.BlockSpec(memory_space=pltpu.SMEM)
    hbm = pl.BlockSpec(memory_space=pl.ANY)
    dma = pltpu.SemaphoreType.DMA
    f32 = lambda *shape: pltpu.VMEM(shape, F32)
    return pl.pallas_call(
        music_kernel,
        out_shape=(
            pltpu.VMEM((BLOCK, 2 * BLOCK), F32),
            pltpu.VMEM((K, BLOCK), F32),
        ),
        in_specs=[hbm, hbm, smem, hbm],
        out_specs=(vmem, vmem),
        scratch_shapes=[
            pltpu.VMEM((256, 128), BF16), pltpu.VMEM((256, 128), BF16), f32(K, BLOCK),
            pltpu.VMEM((9, 256, 128), BF16), pltpu.VMEM((4, 256, 256), BF16),
            pltpu.VMEM((COLS, 1, BLOCK), jnp.int32), pltpu.VMEM((1, BLOCK), jnp.int32),
            pltpu.SMEM((COLS, 1, BLOCK), jnp.int32),
            f32(2, 256, 128), f32(2, 256, 128), f32(2, 384, 128), f32(2, 384, 128), f32(128, 256),
            f32(32, 4, 128), f32(32, 4, 128), f32(32, 4, 128),
            f32(16, 8, 128), f32(16, 8, 128), f32(16, 8, 128),
            f32(16, 4, 128), f32(32, 4, 128), f32(16, 4, 128),
            dma((6, 10)), dma((6,)), dma((2,)), dma((2,)), dma((3, 2)), dma((3, 2)), dma, dma, dma((4,)),
            dma((6,)), dma((6,)),
        ],
        compiler_params=pltpu.CompilerParams(collective_id=0, has_side_effects=True),
        name="music",
    )(own, tail, shift_offsets, start_basis)


def solution(mesh):
    in_specs = (P("row", None, None), P(), P("shift"), P(None, "row"))
    out_specs = (P("row", "shift"), P(None, "row"))
    return jax.shard_map(per_device, mesh=mesh, in_specs=in_specs, out_specs=out_specs, check_vma=False)
```

```python
import jax
import jax.numpy as jnp
from jax import lax
from jax.experimental import pallas as pl
from jax.experimental.pallas import tpu as pltpu
from jax.sharding import PartitionSpec as P

M = 4096
K = 64
SNAPS = 128
SHIFTS = 48
ROWS = 32
COLS = 16
BLOCK = 128
HALF_ROOT = 0.7071067811865476
MESH = pl.DeviceIdType.MESH
HIGHEST = lax.Precision.HIGHEST
F32 = jnp.float32
BF16 = jnp.bfloat16


def far_first(n):
    return sorted(range(n), key=lambda d: -min(d, n - d))


def plane_peers(r):
    x, y = lax.div(r, 8), lax.rem(r, 8)
    xs = [lax.rem(x + a, 4) * 8 for a in range(4)]
    ys = [lax.rem(y + b, 8) for b in range(8)]
    order = sorted(
        ((a, b) for a in range(4) for b in range(8) if a or b),
        key=lambda d: -min(d[0], 4 - d[0]) - min(d[1], 8 - d[1]),
    )
    return [xs[a] + ys[b] for a, b in order]


def line_peers(t):
    z, core = lax.div(t, 2), lax.rem(t, 2)
    zs = [lax.rem(z + a, 8) * 2 for a in range(8)]
    cores = [core, 1 - core]
    return [zs[a] + cores[b] for a in far_first(8) for b in (1, 0) if a or b]


def signal_peers(barrier, rows, places):
    for dest in rows:
        pl.semaphore_signal(barrier, inc=1, device_id={"row": dest}, device_id_type=MESH)
    for dest in places:
        pl.semaphore_signal(barrier, inc=1, device_id={"shift": dest}, device_id_type=MESH)


def lower_inverse(gram):
    lanes = lax.broadcasted_iota(jnp.int32, (8, 128), 1)
    subs = lax.broadcasted_iota(jnp.int32, (8, 128), 0)
    rows = [gram[8 * i : 8 * i + 8] + jnp.where(lanes == subs + 8 * i, 1.0, 0.0) for i in range(8)]
    out = []
    for b in range(8):
        cols = [
            {i: jnp.broadcast_to(rows[i][:, 64 + 8 * b + j : 65 + 8 * b + j], (8, 128)) for i in range(b, 8)}
            for j in range(8)
        ]
        scale = jnp.zeros((8, 128), F32)
        for l in range(8):
            cols[l][b] = jnp.where(lanes < 128 + subs, cols[l][b], 0.0)
        for j in range(8):
            root = jnp.broadcast_to(lax.rsqrt(cols[j][b])[j : j + 1], (8, 128))
            inverse = root * root
            scale = jnp.where(subs == j, root, scale)
            lead = jnp.broadcast_to(rows[b][j : j + 1], (8, 128))
            heads = {l: jnp.broadcast_to(cols[l][b][j : j + 1], (8, 128)) for l in range(j + 1, 8)}
            below = jnp.where(subs > j, cols[j][b], 0.0)
            for l in range(j + 1, 8):
                cols[l][b] = cols[l][b] - (below * heads[l]) * inverse
            rows[b] = rows[b] - (below * lead) * inverse
            for i in range(b + 1, 8):
                factor = cols[j][i] * inverse
                rows[i] = rows[i] - factor * lead
                for l in range(j + 1, 8):
                    cols[l][i] = cols[l][i] - factor * heads[l]
        out.append(rows[b] * scale)
    return jnp.concatenate(out, 0)[:, :64]


def packed_places():
    lanes = lax.broadcasted_iota(jnp.int32, (8, 128), 1)
    subs = lax.broadcasted_iota(jnp.int32, (8, 128), 0)
    group = sum(jnp.where(lanes >= 32 * g, 1, 0) for g in (1, 2, 3))
    return lanes, subs + 8 * group, lanes - 32 * group


def packed_gram(x):
    lanes, row, column = packed_places()

    def repeated(a, b):
        return lax.dot_general(
            a, jnp.concatenate([b] * 4, 0), (((1,), (1,)), ((), ())), precision=HIGHEST, preferred_element_type=F32
        )

    def packed(tiles):
        out = tiles[24:32]
        for g in (2, 1, 0):
            out = jnp.where(lanes < 32 * (g + 1), tiles[8 * g : 8 * g + 8], out)
        return out

    first, second = repeated(x, x[:32]), repeated(x[32:], x[32:])
    last = packed(second)
    mixed = jnp.where(row >= column, packed(first[:32]), last)
    return packed(first[32:]), mixed, jnp.sum(jnp.where(row == column, last, 0.0), axis=0, keepdims=True)


def unpacked_gram(corner, mixed, diagonal):
    lanes, row, column = packed_places()
    same = row == column
    upper = jnp.where(row > column, mixed, jnp.where(same, 0.5 * mixed, 0.0))
    lower = jnp.where(row < column, mixed, jnp.where(same, 0.5 * diagonal, 0.0))
    top, bottom = [], []
    for g in range(4):
        back = (128 - 32 * g) % 128
        top.append(jnp.where(lanes < 32, pltpu.roll(upper, back, 1), 0.0))
        left, right = pltpu.roll(corner, back, 1), pltpu.roll(lower, (back + 32) % 128, 1)
        bottom.append(jnp.where(lanes < 32, left, jnp.where(lanes < 64, right, 0.0)))
    half = jnp.concatenate(top + bottom, 0)[:, :K]
    return jnp.concatenate([jnp.zeros((K, K), F32), half + half.T], 1)


def padded_gram(x):
    both = jnp.concatenate([jnp.zeros_like(x), x], 0)
    return lax.dot_general(x, both, (((1,), (1,)), ((), ())), precision=HIGHEST, preferred_element_type=F32)


def selection(top, flipped):
    out = lax.broadcasted_iota(jnp.int32, (2 * BLOCK, 2 * BLOCK), 0)
    src = lax.broadcasted_iota(jnp.int32, (2 * BLOCK, 2 * BLOCK), 1)
    second = out >= BLOCK
    sensor = jnp.where(second, out - BLOCK, out)
    if flipped:
        sensor = BLOCK - 1 - sensor
    straight = jnp.where(second, 2 * sensor + 1, 2 * sensor)
    crossed = jnp.where(second, 2 * sensor, 2 * sensor + 1)
    minus = second if not flipped else jnp.logical_not(second)
    upper = jnp.where(src == straight, 1.0, 0.0)
    lower = jnp.where(src == crossed, jnp.where(minus, -1.0, 1.0), 0.0)
    return jnp.where(top, upper, lower).astype(BF16)


def music_kernel(
    own_any, tail_any, offs_ref, start_any, cov_ref, mapped_ref, gram_ref,
    own_ref, tail_ref, start_ref,
    got, picks, offs_all, offs_near, offs_now,
    row_w, row_m, col_w, col_m, acc,
    part1, land1, map1, part2, land2, sum2, part3, land3, sum3, partd, landd,
    wide_send, wide_recv, pair_send, pair_recv, near_send, near_recv, offs_send, offs_recv, local_sem,
    send_sem, recv_sem,
):
    r = lax.axis_index("row")
    t = lax.axis_index("shift")
    x, y = lax.div(r, 8), lax.rem(r, 8)
    z, core = lax.div(t, 2), lax.rem(t, 2)
    rows, places = plane_peers(r), line_peers(t)
    column_rows = [x * 8 + lax.rem(y + b, 8) for b in far_first(8) if b]
    bring_own = pltpu.make_async_copy(own_any, own_ref, local_sem.at[1])
    bring_own.start()
    barrier = pltpu.get_barrier_semaphore()
    signal_peers(barrier, rows, places)
    bring_tail = pltpu.make_async_copy(tail_any, tail_ref, local_sem.at[2])
    bring_tail.start()
    bring_start = pltpu.make_async_copy(start_any, start_ref, local_sem.at[3])
    bring_start.start()

    lane = lax.broadcasted_iota(jnp.int32, (1, BLOCK), 1)
    offs_near[...] = jnp.where(lane == 0, offs_ref[0], jnp.where(lane == 1, offs_ref[1], offs_ref[2]))
    half = pl.ds(pl.multiple_of(core * BLOCK, BLOCK), BLOCK)
    other = pl.ds(pl.multiple_of((1 - core) * BLOCK, BLOCK), BLOCK)
    piece = pl.ds(pl.multiple_of(t * 16, 16), 16)
    bring_own.wait()
    pl.semaphore_wait(barrier, ROWS - 1 + COLS - 1)

    slots = []
    for group in range(2):
        if group == 0:
            blocks = (4 * z + 2, 2 * t + 1, 4 * z + 4 * core)
        else:
            blocks = (30 - 4 * z, 31 - 2 * t, 32 - 4 * z - 4 * core)
        for place, block in enumerate(blocks):
            inside = block < ROWS
            bx, by = lax.div(block, 8), lax.rem(block, 8)
            source = block == r
            column = inside & (x == bx) & (y != by)
            opposite = inside & (x == lax.rem(bx + 2, 4)) & (y == by)
            slots.append((3 + 3 * group + place, block, source, column, opposite))

    def shared(slot):
        return slot % 3 == 0

    def wide(slot, k, dest, from_own=False):
        src, dst = own_ref if from_own else got.at[slot], got.at[slot]
        if shared(slot):
            src, dst = src.at[half], dst.at[half]
        return pltpu.make_async_remote_copy(
            src_ref=src,
            dst_ref=dst,
            send_sem=wide_send.at[slot - 3, k],
            recv_sem=wide_recv.at[slot - 3],
            device_id={"row": dest},
            device_id_type=MESH,
        )

    def pair(slot, part):
        return pltpu.make_async_remote_copy(
            src_ref=got.at[slot, part],
            dst_ref=got.at[slot, part],
            send_sem=pair_send.at[slot // 3 - 1],
            recv_sem=pair_recv.at[slot // 3 - 1],
            device_id={"shift": t + 1 - 2 * core},
            device_id_type=MESH,
        )

    def along_y(slot, from_own=False):
        for i, dest in enumerate(column_rows):
            wide(slot, i, dest, from_own).start()

    def along_x(slot, from_own=False):
        wide(slot, 8, lax.rem(x + 1, 4) * 8 + y, from_own).start()
        wide(slot, 9, lax.rem(x + 3, 4) * 8 + y, from_own).start()

    for slot, block, source, column, opposite in slots:
        @pl.when(source)
        def _():
            wide(slot, 7, lax.rem(x + 2, 4) * 8 + y, True).start()
            along_y(slot, True)
            along_x(slot, True)

    def near(slot, dest):
        return pltpu.make_async_remote_copy(
            src_ref=own_ref.at[piece],
            dst_ref=got.at[slot, piece],
            send_sem=near_send.at[slot, 0],
            recv_sem=near_recv.at[slot, 0],
            device_id={"row": dest},
            device_id_type=MESH,
        )

    def pass_on(slot, part, dest):
        return pltpu.make_async_remote_copy(
            src_ref=got.at[slot, part],
            dst_ref=got.at[slot, part],
            send_sem=near_send.at[slot, 1],
            recv_sem=near_recv.at[slot, 1],
            device_id={"shift": dest},
            device_id_type=MESH,
        )

    sends_near = (r >= 1, None, (r >= 1) & (r != 16))
    gets_near = (r != 31, None, (r != 0) & (r != 16))

    def when(condition, body):
        if condition is None:
            body()
        else:
            pl.when(condition)(body)

    for slot, dest in enumerate((r - 1, 31 - r, 32 - r)):
        when(sends_near[slot], lambda: near(slot, dest).start())

    def offs_copy(dest):
        return pltpu.make_async_remote_copy(
            src_ref=offs_near,
            dst_ref=offs_all.at[t],
            send_sem=offs_send,
            recv_sem=offs_recv,
            device_id={"shift": dest},
            device_id_type=MESH,
        )

    for dest in places:
        offs_copy(dest).start()
    offs_all[t] = offs_near[...]

    picks[0] = selection(r < ROWS // 2, False)
    picks[1] = selection(r < ROWS // 2, True)
    picks[2] = selection(t < COLS // 2, False)
    picks[3] = selection(t < COLS // 2, True)
    acc[...] = jnp.zeros_like(acc)
    bring_tail.wait()
    bring_start.wait()

    for slot, block, source, column, opposite in slots:
        @pl.when(source)
        def _():
            got[slot] = own_ref[...]

    def from_tail(slot):
        def body():
            got[slot] = tail_ref[...]

        return body

    pl.when(r == 31)(from_tail(0))
    pl.when(r == 0)(from_tail(2))
    pl.when(t == 15)(from_tail(5))
    pl.when(t == 0)(from_tail(8))

    @pl.when(r == 16)
    def _():
        got[2] = own_ref[...]

    def put(window, pick, place, block):
        both = jnp.dot(picks[pick], block, preferred_element_type=F32) * HALF_ROOT
        span = pl.ds(pl.multiple_of(place * BLOCK, BLOCK), BLOCK)
        window[0, span, :] = both[:BLOCK]
        window[1, span, :] = both[BLOCK:]

    put(row_w, 0, 0, own_ref[...])

    for slot, block, source, column, opposite in slots:
        @pl.when(opposite)
        def _():
            wide(slot, 0, r).wait_recv()
            along_y(slot)

    for slot in range(3):
        def body():
            near(slot, r).wait_recv()

            for dest in places:
                pass_on(slot, piece, dest).start()

        when(gets_near[slot], body)

    for slot, block, source, column, opposite in slots:
        @pl.when(column)
        def _():
            wide(slot, 0, r).wait_recv()
            along_x(slot)

    for slot, block, source, column, opposite in slots:
        if shared(slot):
            waits = jnp.logical_not(source | column | opposite)
            pl.when(waits)(lambda: wide(slot, 0, r).wait_recv())
            pl.when(jnp.logical_not(source))(lambda: pair(slot, half).start())

    every_offs = offs_all.at[pl.ds(0, COLS - 1)]
    whole_offs = pltpu.make_async_remote_copy(
        src_ref=every_offs,
        dst_ref=every_offs,
        send_sem=offs_send,
        recv_sem=offs_recv,
        device_id={"row": r},
        device_id_type=MESH,
    )
    whole_offs.wait_recv()
    to_scalar = pltpu.make_async_copy(offs_all, offs_now, local_sem.at[0])
    to_scalar.start()

    many = pl.ds(0, 16 * (COLS - 1))
    for slot in range(3):
        when(gets_near[slot], lambda: pass_on(slot, many, t).wait_recv())
    put(row_w, 0, 1, got[0])
    put(row_m, 1, 0, got[2])
    put(row_m, 1, 1, got[1])

    for slot, block, source, column, opposite in slots:
        if not shared(slot):
            waits = (block < ROWS) & jnp.logical_not(source | column | opposite)
            pl.when(waits)(lambda: wide(slot, 0, r).wait_recv())
    put(col_w, 2, 1, got[4])
    put(col_m, 3, 1, got[7])
    put(col_w, 2, 2 * core, got[5])
    put(col_m, 3, 2 * core, got[8])
    for slot, block, source, column, opposite in slots:
        if shared(slot):
            pl.when(jnp.logical_not(source))(lambda: pair(slot, other).wait_recv())
    put(col_w, 2, 2 - 2 * core, got[3])
    put(col_m, 3, 2 - 2 * core, got[6])
    to_scalar.wait()

    def pairs(window, mirror, offset, count):
        parts = []
        for c in range(2):
            a = window[c, pl.ds(offset, count), :]
            b = mirror[c, pl.ds(BLOCK - offset, count), :]
            parts.append((a + b).astype(BF16))
        return parts

    def some(i, c):
        lhs, rhs = [], []
        for j in range(12):
            offset = offs_now[i * 4 + j // 3, 0, j % 3]
            lhs += pairs(row_w, row_m, offset, BLOCK)
            rhs += pairs(col_w, col_m, offset, 2 * BLOCK)
        acc[...] += lax.dot_general(
            jnp.concatenate(lhs, 1), jnp.concatenate(rhs, 1), (((1,), (1,)), ((), ())), preferred_element_type=F32
        )
        return c

    lax.fori_loop(0, 4, some, 0)
    cov = acc[...] * (1.0 / (SNAPS * SHIFTS))
    cov_ref[...] = cov

    first = jnp.dot(start_ref[...], cov, precision=HIGHEST, preferred_element_type=F32)
    for c in range(2):
        for a in range(16):
            part1[16 * c + a] = first[4 * a : 4 * a + 4, BLOCK * c : BLOCK * c + BLOCK]

    def copy(src, dst, phase, where):
        return pltpu.make_async_remote_copy(
            src_ref=src,
            dst_ref=dst,
            send_sem=send_sem.at[phase],
            recv_sem=recv_sem.at[phase],
            device_id=where,
            device_id_type=MESH,
        )

    def total(phase, buffer, count):
        every = buffer.at[pl.ds(0, count)]
        return copy(every, every, phase, {"row": r})

    for dest in rows:
        copy(part1.at[dest], land1.at[r], 0, {"row": dest}).start()
    land1[r] = part1[r]
    total(0, land1, ROWS - 1).wait_recv()
    map1[r] = jnp.sum(land1[...], axis=0)

    for dest in rows:
        copy(map1.at[r], map1.at[r], 1, {"row": dest}).start()
    total(1, map1, ROWS - 1).wait_recv()
    mapped = jnp.concatenate(
        [jnp.concatenate([map1[16 * c + a] for a in range(16)], 0) for c in range(2)], 1
    )

    gram1 = padded_gram(mapped)
    second = lax.dot_general(
        mapped, cov_ref[...], (((1,), (1,)), ((), ())), precision=HIGHEST, preferred_element_type=F32
    )
    for a in range(8):
        part2[a] = second[8 * a : 8 * a + 8]
        part2[8 + a] = gram1[8 * a : 8 * a + 8]

    for dest in places:
        copy(part2.at[dest], land2.at[t], 2, {"shift": dest}).start()
    land2[t] = part2[t]
    total(2, land2, COLS - 1).wait_recv()
    sum2[t] = jnp.sum(land2[...], axis=0)

    for dest in places:
        copy(sum2.at[t], sum2.at[t], 3, {"shift": dest}).start()
    total(3, sum2, COLS - 1).wait_recv()
    factor1 = lower_inverse(sum2[8:16].reshape(K, BLOCK))
    mapped2 = jnp.dot(factor1, sum2[0:8].reshape(K, BLOCK), precision=HIGHEST, preferred_element_type=F32)
    corner, mixed, diagonal = packed_gram(mapped2)
    part3[...] = jnp.where(core == 0, corner, mixed)
    partd[...] = diagonal
    for dest in rows:
        copy(part3, land3.at[r], 4, {"row": dest}).start()
    for dest in rows:
        copy(partd, landd.at[r], 6, {"row": dest}).start()
    land3[r] = part3[...]
    landd[r] = partd[...]
    total(4, land3, ROWS - 1).wait_recv()
    sum3[core] = jnp.sum(land3[...], axis=0)
    halves = copy(sum3.at[core], sum3.at[core], 5, {"shift": t + 1 - 2 * core})
    halves.start()
    total(6, landd, ROWS - 1).wait_recv()
    diagonal = jnp.broadcast_to(jnp.sum(landd[...], axis=0), (8, 128))
    halves.wait_recv()
    whole = unpacked_gram(sum3[0], sum3[1], diagonal)
    mapped_ref[...] = mapped2
    gram_ref[...] = whole

    for slot, block, source, column, opposite in slots:
        def drain(low, high):
            def done(k, c):
                wide(slot, k, r).wait_send()
                return c

            lax.fori_loop(low, high, done, 0)

        pl.when(source)(lambda: drain(0, 10))
        pl.when(column)(lambda: drain(8, 10))
        pl.when(opposite)(lambda: drain(0, 7))
        if shared(slot):
            pl.when(jnp.logical_not(source))(lambda: pair(slot, half).wait_send())
    for slot in range(3):
        when(sends_near[slot], lambda: near(slot, r).wait_send())
        when(gets_near[slot], lambda: pass_on(slot, many, t).wait_send())
    whole_offs.wait_send()
    total(0, land1, ROWS - 1).wait_send()
    total(1, map1, ROWS - 1).wait_send()
    total(2, land2, COLS - 1).wait_send()
    total(3, sum2, COLS - 1).wait_send()
    total(4, land3, ROWS - 1).wait_send()
    halves.wait_send()
    total(6, landd, ROWS - 1).wait_send()


def finish_kernel(cov_ref, mapped_ref, gram_ref, cov_out, basis_ref, sem):
    write = pltpu.make_async_copy(cov_ref, cov_out, sem)
    write.start()
    basis_ref[...] = jnp.dot(
        lower_inverse(gram_ref[...]), mapped_ref[...], precision=HIGHEST, preferred_element_type=F32
    )
    write.wait()


def per_device(snapshots, tail_sensors, shift_offsets, start_basis):
    own = snapshots.reshape(2 * BLOCK, SNAPS)
    tail = tail_sensors.reshape(2 * BLOCK, SNAPS)
    vmem = pl.BlockSpec(memory_space=pltpu.VMEM)
    smem = pl.BlockSpec(memory_space=pltpu.SMEM)
    hbm = pl.BlockSpec(memory_space=pl.ANY)
    dma = pltpu.SemaphoreType.DMA
    f32 = lambda *shape: pltpu.VMEM(shape, F32)
    cov, mapped, gram = pl.pallas_call(
        music_kernel,
        out_shape=(
            pltpu.VMEM((BLOCK, 2 * BLOCK), F32),
            pltpu.VMEM((K, BLOCK), F32),
            pltpu.VMEM((K, BLOCK), F32),
        ),
        in_specs=[hbm, hbm, smem, hbm],
        out_specs=(vmem, vmem, vmem),
        scratch_shapes=[
            pltpu.VMEM((256, 128), BF16), pltpu.VMEM((256, 128), BF16), f32(K, BLOCK),
            pltpu.VMEM((9, 256, 128), BF16), pltpu.VMEM((4, 256, 256), BF16),
            pltpu.VMEM((COLS, 1, BLOCK), jnp.int32), pltpu.VMEM((1, BLOCK), jnp.int32),
            pltpu.SMEM((COLS, 1, BLOCK), jnp.int32),
            f32(2, 256, 128), f32(2, 256, 128), f32(2, 384, 128), f32(2, 384, 128), f32(128, 256),
            f32(32, 4, 128), f32(32, 4, 128), f32(32, 4, 128),
            f32(16, 8, 128), f32(16, 8, 128), f32(16, 8, 128),
            f32(8, 128), f32(32, 8, 128), f32(2, 8, 128), f32(1, 128), f32(32, 1, 128),
            dma((6, 10)), dma((6,)), dma((2,)), dma((2,)), dma((3, 2)), dma((3, 2)), dma, dma, dma((4,)),
            dma((7,)), dma((7,)),
        ],
        compiler_params=pltpu.CompilerParams(collective_id=0, has_side_effects=True),
        name="music",
    )(own, tail, shift_offsets, start_basis)
    return pl.pallas_call(
        finish_kernel,
        out_shape=(
            jax.ShapeDtypeStruct((BLOCK, 2 * BLOCK), F32),
            jax.ShapeDtypeStruct((K, BLOCK), F32),
        ),
        in_specs=[vmem, vmem, vmem],
        out_specs=(hbm, vmem),
        scratch_shapes=[dma],
        name="finish",
    )(*(pltpu.with_memory_space_constraint(x, pltpu.VMEM) for x in (cov, mapped, gram)))


def solution(mesh):
    in_specs = (P("row", None, None), P(), P("shift"), P(None, "row"))
    out_specs = (P("row", "shift"), P(None, "row"))
    return jax.shard_map(per_device, mesh=mesh, in_specs=in_specs, out_specs=out_specs, check_vma=False)
```

```python
import jax
import jax.numpy as jnp
from jax import lax
from jax.experimental import pallas as pl
from jax.experimental.pallas import tpu as pltpu
from jax.sharding import PartitionSpec as P

M = 4096
K = 64
SNAPS = 128
SHIFTS = 48
ROWS = 32
COLS = 16
BLOCK = 128
HALF_ROOT = 0.7071067811865476
MESH = pl.DeviceIdType.MESH
HIGHEST = lax.Precision.HIGHEST
F32 = jnp.float32
BF16 = jnp.bfloat16


def far_first(n):
    return sorted(range(n), key=lambda d: -min(d, n - d))


def plane_peers(r):
    x, y = lax.div(r, 8), lax.rem(r, 8)
    xs = [lax.rem(x + a, 4) * 8 for a in range(4)]
    ys = [lax.rem(y + b, 8) for b in range(8)]
    order = sorted(
        ((a, b) for a in range(4) for b in range(8) if a or b),
        key=lambda d: -min(d[0], 4 - d[0]) - min(d[1], 8 - d[1]),
    )
    return [xs[a] + ys[b] for a, b in order]


def line_peers(t):
    z, core = lax.div(t, 2), lax.rem(t, 2)
    zs = [lax.rem(z + a, 8) * 2 for a in range(8)]
    cores = [core, 1 - core]
    return [zs[a] + cores[b] for a in far_first(8) for b in (1, 0) if a or b]


def signal_peers(barrier, rows, places):
    for dest in rows:
        pl.semaphore_signal(barrier, inc=1, device_id={"row": dest}, device_id_type=MESH)
    for dest in places:
        pl.semaphore_signal(barrier, inc=1, device_id={"shift": dest}, device_id_type=MESH)


def lower_inverse(gram):
    lanes = lax.broadcasted_iota(jnp.int32, (8, 128), 1)
    subs = lax.broadcasted_iota(jnp.int32, (8, 128), 0)
    rows = [gram[8 * i : 8 * i + 8] + jnp.where(lanes == subs + 8 * i, 1.0, 0.0) for i in range(8)]
    out = []
    for b in range(8):
        cols = [
            {i: jnp.broadcast_to(rows[i][:, 64 + 8 * b + j : 65 + 8 * b + j], (8, 128)) for i in range(b, 8)}
            for j in range(8)
        ]
        scale = jnp.zeros((8, 128), F32)
        for l in range(8):
            cols[l][b] = jnp.where(lanes < 128 + subs, cols[l][b], 0.0)
        for j in range(8):
            root = jnp.broadcast_to(lax.rsqrt(cols[j][b])[j : j + 1], (8, 128))
            inverse = root * root
            scale = jnp.where(subs == j, root, scale)
            lead = jnp.broadcast_to(rows[b][j : j + 1], (8, 128))
            heads = {l: jnp.broadcast_to(cols[l][b][j : j + 1], (8, 128)) for l in range(j + 1, 8)}
            below = jnp.where(subs > j, cols[j][b], 0.0)
            for l in range(j + 1, 8):
                cols[l][b] = cols[l][b] - (below * heads[l]) * inverse
            rows[b] = rows[b] - (below * lead) * inverse
            for i in range(b + 1, 8):
                factor = cols[j][i] * inverse
                rows[i] = rows[i] - factor * lead
                for l in range(j + 1, 8):
                    cols[l][i] = cols[l][i] - factor * heads[l]
        out.append(rows[b] * scale)
    return jnp.concatenate(out, 0)[:, :64]


def packed_places():
    lanes = lax.broadcasted_iota(jnp.int32, (8, 128), 1)
    subs = lax.broadcasted_iota(jnp.int32, (8, 128), 0)
    group = sum(jnp.where(lanes >= 32 * g, 1, 0) for g in (1, 2, 3))
    return lanes, subs + 8 * group, lanes - 32 * group


def packed_gram(x):
    lanes, row, column = packed_places()

    def repeated(a, b):
        return lax.dot_general(
            a, jnp.concatenate([b] * 4, 0), (((1,), (1,)), ((), ())), precision=HIGHEST, preferred_element_type=F32
        )

    def packed(tiles):
        out = tiles[24:32]
        for g in (2, 1, 0):
            out = jnp.where(lanes < 32 * (g + 1), tiles[8 * g : 8 * g + 8], out)
        return out

    first, second = repeated(x, x[:32]), repeated(x[32:], x[32:])
    last = packed(second)
    mixed = jnp.where(row >= column, packed(first[:32]), last)
    return packed(first[32:]), mixed, jnp.sum(jnp.where(row == column, last, 0.0), axis=0, keepdims=True)


def unpacked_gram(corner, mixed, diagonal):
    lanes, row, column = packed_places()
    same = row == column
    upper = jnp.where(row > column, mixed, jnp.where(same, 0.5 * mixed, 0.0))
    lower = jnp.where(row < column, mixed, jnp.where(same, 0.5 * diagonal, 0.0))
    top, bottom = [], []
    for g in range(4):
        back = (128 - 32 * g) % 128
        top.append(jnp.where(lanes < 32, pltpu.roll(upper, back, 1), 0.0))
        left, right = pltpu.roll(corner, back, 1), pltpu.roll(lower, (back + 32) % 128, 1)
        bottom.append(jnp.where(lanes < 32, left, jnp.where(lanes < 64, right, 0.0)))
    half = jnp.concatenate(top + bottom, 0)[:, :K]
    return jnp.concatenate([jnp.zeros((K, K), F32), half + half.T], 1)


def selection(top, flipped):
    out = lax.broadcasted_iota(jnp.int32, (2 * BLOCK, 2 * BLOCK), 0)
    src = lax.broadcasted_iota(jnp.int32, (2 * BLOCK, 2 * BLOCK), 1)
    second = out >= BLOCK
    sensor = jnp.where(second, out - BLOCK, out)
    if flipped:
        sensor = BLOCK - 1 - sensor
    straight = jnp.where(second, 2 * sensor + 1, 2 * sensor)
    crossed = jnp.where(second, 2 * sensor, 2 * sensor + 1)
    minus = second if not flipped else jnp.logical_not(second)
    upper = jnp.where(src == straight, 1.0, 0.0)
    lower = jnp.where(src == crossed, jnp.where(minus, -1.0, 1.0), 0.0)
    return jnp.where(top, upper, lower).astype(BF16)


def music_kernel(
    own_any, tail_any, offs_ref, start_any, cov_ref, mapped_ref, gram_ref,
    own_ref, tail_ref, start_ref,
    got, picks, offs_all, offs_near, offs_now,
    row_w, row_m, col_w, col_m, acc,
    part1, land1, map1, part2, beside, middle, land2, sum2, part3, land3, sum3, partd, landd,
    wide_send, wide_recv, pair_send, pair_recv, near_send, near_recv, offs_send, offs_recv, local_sem,
    send_sem, recv_sem,
):
    r = lax.axis_index("row")
    t = lax.axis_index("shift")
    x, y = lax.div(r, 8), lax.rem(r, 8)
    z, core = lax.div(t, 2), lax.rem(t, 2)
    rows, places = plane_peers(r), line_peers(t)
    column_rows = [x * 8 + lax.rem(y + b, 8) for b in far_first(8) if b]
    bring_own = pltpu.make_async_copy(own_any, own_ref, local_sem.at[1])
    bring_own.start()
    barrier = pltpu.get_barrier_semaphore()
    signal_peers(barrier, rows, places)
    bring_tail = pltpu.make_async_copy(tail_any, tail_ref, local_sem.at[2])
    bring_tail.start()
    bring_start = pltpu.make_async_copy(start_any, start_ref, local_sem.at[3])
    bring_start.start()

    lane = lax.broadcasted_iota(jnp.int32, (1, BLOCK), 1)
    offs_near[...] = jnp.where(lane == 0, offs_ref[0], jnp.where(lane == 1, offs_ref[1], offs_ref[2]))
    half = pl.ds(pl.multiple_of(core * BLOCK, BLOCK), BLOCK)
    other = pl.ds(pl.multiple_of((1 - core) * BLOCK, BLOCK), BLOCK)
    piece = pl.ds(pl.multiple_of(t * 16, 16), 16)
    bring_own.wait()
    pl.semaphore_wait(barrier, ROWS - 1 + COLS - 1)

    slots = []
    for group in range(2):
        if group == 0:
            blocks = (4 * z + 2, 2 * t + 1, 4 * z + 4 * core)
        else:
            blocks = (30 - 4 * z, 31 - 2 * t, 32 - 4 * z - 4 * core)
        for place, block in enumerate(blocks):
            inside = block < ROWS
            bx, by = lax.div(block, 8), lax.rem(block, 8)
            source = block == r
            column = inside & (x == bx) & (y != by)
            opposite = inside & (x == lax.rem(bx + 2, 4)) & (y == by)
            slots.append((3 + 3 * group + place, block, source, column, opposite))

    def shared(slot):
        return slot % 3 == 0

    def wide(slot, k, dest, from_own=False):
        src, dst = own_ref if from_own else got.at[slot], got.at[slot]
        if shared(slot):
            src, dst = src.at[half], dst.at[half]
        return pltpu.make_async_remote_copy(
            src_ref=src,
            dst_ref=dst,
            send_sem=wide_send.at[slot - 3, k],
            recv_sem=wide_recv.at[slot - 3],
            device_id={"row": dest},
            device_id_type=MESH,
        )

    def pair(slot, part):
        return pltpu.make_async_remote_copy(
            src_ref=got.at[slot, part],
            dst_ref=got.at[slot, part],
            send_sem=pair_send.at[slot // 3 - 1],
            recv_sem=pair_recv.at[slot // 3 - 1],
            device_id={"shift": t + 1 - 2 * core},
            device_id_type=MESH,
        )

    def along_y(slot, from_own=False):
        for i, dest in enumerate(column_rows):
            wide(slot, i, dest, from_own).start()

    def along_x(slot, from_own=False):
        wide(slot, 8, lax.rem(x + 1, 4) * 8 + y, from_own).start()
        wide(slot, 9, lax.rem(x + 3, 4) * 8 + y, from_own).start()

    for slot, block, source, column, opposite in slots:
        @pl.when(source)
        def _():
            wide(slot, 7, lax.rem(x + 2, 4) * 8 + y, True).start()
            along_y(slot, True)
            along_x(slot, True)

    def near(slot, dest):
        return pltpu.make_async_remote_copy(
            src_ref=own_ref.at[piece],
            dst_ref=got.at[slot, piece],
            send_sem=near_send.at[slot, 0],
            recv_sem=near_recv.at[slot, 0],
            device_id={"row": dest},
            device_id_type=MESH,
        )

    def pass_on(slot, part, dest):
        return pltpu.make_async_remote_copy(
            src_ref=got.at[slot, part],
            dst_ref=got.at[slot, part],
            send_sem=near_send.at[slot, 1],
            recv_sem=near_recv.at[slot, 1],
            device_id={"shift": dest},
            device_id_type=MESH,
        )

    sends_near = (r >= 1, None, (r >= 1) & (r != 16))
    gets_near = (r != 31, None, (r != 0) & (r != 16))

    def when(condition, body):
        if condition is None:
            body()
        else:
            pl.when(condition)(body)

    for slot, dest in enumerate((r - 1, 31 - r, 32 - r)):
        when(sends_near[slot], lambda: near(slot, dest).start())

    def offs_copy(dest):
        return pltpu.make_async_remote_copy(
            src_ref=offs_near,
            dst_ref=offs_all.at[t],
            send_sem=offs_send,
            recv_sem=offs_recv,
            device_id={"shift": dest},
            device_id_type=MESH,
        )

    for dest in places:
        offs_copy(dest).start()
    offs_all[t] = offs_near[...]

    picks[0] = selection(r < ROWS // 2, False)
    picks[1] = selection(r < ROWS // 2, True)
    picks[2] = selection(t < COLS // 2, False)
    picks[3] = selection(t < COLS // 2, True)
    acc[...] = jnp.zeros_like(acc)
    bring_tail.wait()
    bring_start.wait()

    for slot, block, source, column, opposite in slots:
        @pl.when(source)
        def _():
            got[slot] = own_ref[...]

    def from_tail(slot):
        def body():
            got[slot] = tail_ref[...]

        return body

    pl.when(r == 31)(from_tail(0))
    pl.when(r == 0)(from_tail(2))
    pl.when(t == 15)(from_tail(5))
    pl.when(t == 0)(from_tail(8))

    @pl.when(r == 16)
    def _():
        got[2] = own_ref[...]

    def put(window, pick, place, block):
        both = jnp.dot(picks[pick], block, preferred_element_type=F32) * HALF_ROOT
        span = pl.ds(pl.multiple_of(place * BLOCK, BLOCK), BLOCK)
        window[0, span, :] = both[:BLOCK]
        window[1, span, :] = both[BLOCK:]

    put(row_w, 0, 0, own_ref[...])

    for slot, block, source, column, opposite in slots:
        @pl.when(opposite)
        def _():
            wide(slot, 0, r).wait_recv()
            along_y(slot)

    for slot in range(3):
        def body():
            near(slot, r).wait_recv()

            for dest in places:
                pass_on(slot, piece, dest).start()

        when(gets_near[slot], body)

    for slot, block, source, column, opposite in slots:
        @pl.when(column)
        def _():
            wide(slot, 0, r).wait_recv()
            along_x(slot)

    for slot, block, source, column, opposite in slots:
        if shared(slot):
            waits = jnp.logical_not(source | column | opposite)
            pl.when(waits)(lambda: wide(slot, 0, r).wait_recv())
            pl.when(jnp.logical_not(source))(lambda: pair(slot, half).start())

    every_offs = offs_all.at[pl.ds(0, COLS - 1)]
    whole_offs = pltpu.make_async_remote_copy(
        src_ref=every_offs,
        dst_ref=every_offs,
        send_sem=offs_send,
        recv_sem=offs_recv,
        device_id={"row": r},
        device_id_type=MESH,
    )
    whole_offs.wait_recv()
    to_scalar = pltpu.make_async_copy(offs_all, offs_now, local_sem.at[0])
    to_scalar.start()

    many = pl.ds(0, 16 * (COLS - 1))
    for slot in range(3):
        when(gets_near[slot], lambda: pass_on(slot, many, t).wait_recv())
    put(row_w, 0, 1, got[0])
    put(row_m, 1, 0, got[2])
    put(row_m, 1, 1, got[1])

    for slot, block, source, column, opposite in slots:
        if not shared(slot):
            waits = (block < ROWS) & jnp.logical_not(source | column | opposite)
            pl.when(waits)(lambda: wide(slot, 0, r).wait_recv())
    put(col_w, 2, 1, got[4])
    put(col_m, 3, 1, got[7])
    put(col_w, 2, 2 * core, got[5])
    put(col_m, 3, 2 * core, got[8])
    for slot, block, source, column, opposite in slots:
        if shared(slot):
            pl.when(jnp.logical_not(source))(lambda: pair(slot, other).wait_recv())
    put(col_w, 2, 2 - 2 * core, got[3])
    put(col_m, 3, 2 - 2 * core, got[6])
    to_scalar.wait()

    def pairs(window, mirror, offset, count):
        parts = []
        for c in range(2):
            a = window[c, pl.ds(offset, count), :]
            b = mirror[c, pl.ds(BLOCK - offset, count), :]
            parts.append((a + b).astype(BF16))
        return parts

    def some(i, c):
        lhs, rhs = [], []
        for j in range(12):
            offset = offs_now[i * 4 + j // 3, 0, j % 3]
            lhs += pairs(row_w, row_m, offset, BLOCK)
            rhs += pairs(col_w, col_m, offset, 2 * BLOCK)
        acc[...] += lax.dot_general(
            jnp.concatenate(lhs, 1), jnp.concatenate(rhs, 1), (((1,), (1,)), ((), ())), preferred_element_type=F32
        )
        return c

    lax.fori_loop(0, 4, some, 0)
    cov = acc[...] * (1.0 / (SNAPS * SHIFTS))
    cov_ref[...] = cov

    first = jnp.dot(start_ref[...], cov, precision=HIGHEST, preferred_element_type=F32)
    for c in range(2):
        for a in range(16):
            part1[16 * c + a] = first[4 * a : 4 * a + 4, BLOCK * c : BLOCK * c + BLOCK]

    def copy(src, dst, phase, where):
        return pltpu.make_async_remote_copy(
            src_ref=src,
            dst_ref=dst,
            send_sem=send_sem.at[phase],
            recv_sem=recv_sem.at[phase],
            device_id=where,
            device_id_type=MESH,
        )

    def total(phase, buffer, count):
        every = buffer.at[pl.ds(0, count)]
        return copy(every, every, phase, {"row": r})

    for dest in rows:
        copy(part1.at[dest], land1.at[r], 0, {"row": dest}).start()
    land1[r] = part1[r]
    total(0, land1, ROWS - 1).wait_recv()
    map1[r] = jnp.sum(land1[...], axis=0)

    for dest in rows:
        copy(map1.at[r], map1.at[r], 1, {"row": dest}).start()
    total(1, map1, ROWS - 1).wait_recv()
    mapped = jnp.concatenate(
        [jnp.concatenate([map1[16 * c + a] for a in range(16)], 0) for c in range(2)], 1
    )

    lanes = lax.broadcasted_iota(jnp.int32, (8, BLOCK), 1)
    gram1 = lax.dot_general(
        mapped, jnp.concatenate([mapped, mapped], 0), (((1,), (1,)), ((), ())), precision=HIGHEST, preferred_element_type=F32
    )
    second = lax.dot_general(
        mapped, cov_ref[...], (((1,), (1,)), ((), ())), precision=HIGHEST, preferred_element_type=F32
    )
    for h in range(2):
        for i in range(4):
            part2[h, i] = second[32 * h + 8 * i : 32 * h + 8 * i + 8]
        for i in range(2):
            a = 16 * h + 8 * i
            part2[h, 4 + i] = jnp.where(lanes < K, gram1[a : a + 8], gram1[32 + a : 40 + a])
    partner = {"shift": t + 1 - 2 * core}
    meet = copy(part2.at[1 - core], beside, 2, partner)
    meet.start()
    meet.wait_recv()
    middle[...] = part2[core] + beside[...]
    for b in far_first(8):
        if b:
            copy(middle, land2.at[z], 3, {"shift": lax.rem(z + b, 8) * 2 + core}).start()
    land2[z] = middle[...]
    total(3, land2, 7).wait_recv()
    sum2[core] = jnp.sum(land2[...], axis=0)
    swap = copy(sum2.at[core], sum2.at[core], 7, partner)
    swap.start()
    swap.wait_recv()
    tiles = [sum2[h, 4 + i] for h in range(2) for i in range(2)]
    gram1 = jnp.concatenate(
        [jnp.where(lanes < K, 0.0, pltpu.roll(tile, K, 1)) for tile in tiles]
        + [jnp.where(lanes < K, 0.0, tile) for tile in tiles],
        0,
    )
    factor1 = lower_inverse(gram1)
    product = jnp.concatenate([sum2[h, i] for h in range(2) for i in range(4)], 0)
    mapped2 = jnp.dot(factor1, product, precision=HIGHEST, preferred_element_type=F32)
    corner, mixed, diagonal = packed_gram(mapped2)
    part3[...] = jnp.where(core == 0, corner, mixed)
    partd[...] = diagonal
    for dest in rows:
        copy(part3, land3.at[r], 4, {"row": dest}).start()
    for dest in rows:
        copy(partd, landd.at[r], 6, {"row": dest}).start()
    land3[r] = part3[...]
    landd[r] = partd[...]
    total(4, land3, ROWS - 1).wait_recv()
    sum3[core] = jnp.sum(land3[...], axis=0)
    halves = copy(sum3.at[core], sum3.at[core], 5, {"shift": t + 1 - 2 * core})
    halves.start()
    total(6, landd, ROWS - 1).wait_recv()
    diagonal = jnp.broadcast_to(jnp.sum(landd[...], axis=0), (8, 128))
    halves.wait_recv()
    whole = unpacked_gram(sum3[0], sum3[1], diagonal)
    mapped_ref[...] = mapped2
    gram_ref[...] = whole

    for slot, block, source, column, opposite in slots:
        def drain(low, high):
            def done(k, c):
                wide(slot, k, r).wait_send()
                return c

            lax.fori_loop(low, high, done, 0)

        pl.when(source)(lambda: drain(0, 10))
        pl.when(column)(lambda: drain(8, 10))
        pl.when(opposite)(lambda: drain(0, 7))
        if shared(slot):
            pl.when(jnp.logical_not(source))(lambda: pair(slot, half).wait_send())
    for slot in range(3):
        when(sends_near[slot], lambda: near(slot, r).wait_send())
        when(gets_near[slot], lambda: pass_on(slot, many, t).wait_send())
    whole_offs.wait_send()
    total(0, land1, ROWS - 1).wait_send()
    total(1, map1, ROWS - 1).wait_send()
    meet.wait_send()
    total(3, land2, 7).wait_send()
    swap.wait_send()
    total(4, land3, ROWS - 1).wait_send()
    halves.wait_send()
    total(6, landd, ROWS - 1).wait_send()


def finish_kernel(cov_ref, mapped_ref, gram_ref, cov_out, basis_ref, sem):
    write = pltpu.make_async_copy(cov_ref, cov_out, sem)
    write.start()
    basis_ref[...] = jnp.dot(
        lower_inverse(gram_ref[...]), mapped_ref[...], precision=HIGHEST, preferred_element_type=F32
    )
    write.wait()


def per_device(snapshots, tail_sensors, shift_offsets, start_basis):
    own = snapshots.reshape(2 * BLOCK, SNAPS)
    tail = tail_sensors.reshape(2 * BLOCK, SNAPS)
    vmem = pl.BlockSpec(memory_space=pltpu.VMEM)
    smem = pl.BlockSpec(memory_space=pltpu.SMEM)
    hbm = pl.BlockSpec(memory_space=pl.ANY)
    dma = pltpu.SemaphoreType.DMA
    f32 = lambda *shape: pltpu.VMEM(shape, F32)
    cov, mapped, gram = pl.pallas_call(
        music_kernel,
        out_shape=(
            pltpu.VMEM((BLOCK, 2 * BLOCK), F32),
            pltpu.VMEM((K, BLOCK), F32),
            pltpu.VMEM((K, BLOCK), F32),
        ),
        in_specs=[hbm, hbm, smem, hbm],
        out_specs=(vmem, vmem, vmem),
        scratch_shapes=[
            pltpu.VMEM((256, 128), BF16), pltpu.VMEM((256, 128), BF16), f32(K, BLOCK),
            pltpu.VMEM((9, 256, 128), BF16), pltpu.VMEM((4, 256, 256), BF16),
            pltpu.VMEM((COLS, 1, BLOCK), jnp.int32), pltpu.VMEM((1, BLOCK), jnp.int32),
            pltpu.SMEM((COLS, 1, BLOCK), jnp.int32),
            f32(2, 256, 128), f32(2, 256, 128), f32(2, 384, 128), f32(2, 384, 128), f32(128, 256),
            f32(32, 4, 128), f32(32, 4, 128), f32(32, 4, 128),
            f32(2, 6, 8, 128), f32(6, 8, 128), f32(6, 8, 128), f32(8, 6, 8, 128), f32(2, 6, 8, 128),
            f32(8, 128), f32(32, 8, 128), f32(2, 8, 128), f32(1, 128), f32(32, 1, 128),
            dma((6, 10)), dma((6,)), dma((2,)), dma((2,)), dma((3, 2)), dma((3, 2)), dma, dma, dma((4,)),
            dma((8,)), dma((8,)),
        ],
        compiler_params=pltpu.CompilerParams(collective_id=0, has_side_effects=True),
        name="music",
    )(own, tail, shift_offsets, start_basis)
    return pl.pallas_call(
        finish_kernel,
        out_shape=(
            jax.ShapeDtypeStruct((BLOCK, 2 * BLOCK), F32),
            jax.ShapeDtypeStruct((K, BLOCK), F32),
        ),
        in_specs=[vmem, vmem, vmem],
        out_specs=(hbm, vmem),
        scratch_shapes=[dma],
        name="finish",
    )(*(pltpu.with_memory_space_constraint(x, pltpu.VMEM) for x in (cov, mapped, gram)))


def solution(mesh):
    in_specs = (P("row", None, None), P(), P("shift"), P(None, "row"))
    out_specs = (P("row", "shift"), P(None, "row"))
    return jax.shard_map(per_device, mesh=mesh, in_specs=in_specs, out_specs=out_specs, check_vma=False)
```

```python
import jax
import jax.numpy as jnp
from jax import lax
from jax.experimental import pallas as pl
from jax.experimental.pallas import tpu as pltpu
from jax.sharding import PartitionSpec as P

M = 4096
K = 64
SNAPS = 128
SHIFTS = 48
ROWS = 32
COLS = 16
BLOCK = 128
HALF_ROOT = 0.7071067811865476
MESH = pl.DeviceIdType.MESH
HIGHEST = lax.Precision.HIGHEST
F32 = jnp.float32
BF16 = jnp.bfloat16


def far_first(n):
    return sorted(range(n), key=lambda d: -min(d, n - d))


def plane_peers(r):
    x, y = lax.div(r, 8), lax.rem(r, 8)
    xs = [lax.rem(x + a, 4) * 8 for a in range(4)]
    ys = [lax.rem(y + b, 8) for b in range(8)]
    order = sorted(
        ((a, b) for a in range(4) for b in range(8) if a or b),
        key=lambda d: -min(d[0], 4 - d[0]) - min(d[1], 8 - d[1]),
    )
    return [xs[a] + ys[b] for a, b in order]


def line_peers(t):
    z, core = lax.div(t, 2), lax.rem(t, 2)
    zs = [lax.rem(z + a, 8) * 2 for a in range(8)]
    cores = [core, 1 - core]
    return [zs[a] + cores[b] for a in far_first(8) for b in (1, 0) if a or b]


def signal_peers(barrier, rows, places):
    for dest in rows:
        pl.semaphore_signal(barrier, inc=1, device_id={"row": dest}, device_id_type=MESH)
    for dest in places:
        pl.semaphore_signal(barrier, inc=1, device_id={"shift": dest}, device_id_type=MESH)


def lower_inverse(gram):
    lanes = lax.broadcasted_iota(jnp.int32, (8, 128), 1)
    subs = lax.broadcasted_iota(jnp.int32, (8, 128), 0)
    rows = [gram[8 * i : 8 * i + 8] + jnp.where(lanes == subs + 8 * i, 1.0, 0.0) for i in range(8)]
    out = []
    for b in range(8):
        cols = [
            {i: jnp.broadcast_to(rows[i][:, 64 + 8 * b + j : 65 + 8 * b + j], (8, 128)) for i in range(b, 8)}
            for j in range(8)
        ]
        scale = jnp.zeros((8, 128), F32)
        for l in range(8):
            cols[l][b] = jnp.where(lanes < 128 + subs, cols[l][b], 0.0)
        for j in range(8):
            root = jnp.broadcast_to(lax.rsqrt(cols[j][b])[j : j + 1], (8, 128))
            inverse = root * root
            scale = jnp.where(subs == j, root, scale)
            lead = jnp.broadcast_to(rows[b][j : j + 1], (8, 128))
            heads = {l: jnp.broadcast_to(cols[l][b][j : j + 1], (8, 128)) for l in range(j + 1, 8)}
            below = jnp.where(subs > j, cols[j][b], 0.0)
            for l in range(j + 1, 8):
                cols[l][b] = cols[l][b] - (below * heads[l]) * inverse
            rows[b] = rows[b] - (below * lead) * inverse
            for i in range(b + 1, 8):
                factor = cols[j][i] * inverse
                rows[i] = rows[i] - factor * lead
                for l in range(j + 1, 8):
                    cols[l][i] = cols[l][i] - factor * heads[l]
        out.append(rows[b] * scale)
    return jnp.concatenate(out, 0)[:, :64]


def packed_places():
    lanes = lax.broadcasted_iota(jnp.int32, (8, 128), 1)
    subs = lax.broadcasted_iota(jnp.int32, (8, 128), 0)
    group = sum(jnp.where(lanes >= 32 * g, 1, 0) for g in (1, 2, 3))
    return lanes, subs + 8 * group, lanes - 32 * group


def packed_gram(x):
    lanes, row, column = packed_places()

    def repeated(a, b):
        return lax.dot_general(
            a, jnp.concatenate([b] * 4, 0), (((1,), (1,)), ((), ())), precision=HIGHEST, preferred_element_type=F32
        )

    def packed(tiles):
        out = tiles[24:32]
        for g in (2, 1, 0):
            out = jnp.where(lanes < 32 * (g + 1), tiles[8 * g : 8 * g + 8], out)
        return out

    first, second = repeated(x, x[:32]), repeated(x[32:], x[32:])
    last = packed(second)
    mixed = jnp.where(row >= column, packed(first[:32]), last)
    return packed(first[32:]), mixed, jnp.sum(jnp.where(row == column, last, 0.0), axis=0, keepdims=True)


def unpacked_gram(corner, mixed, diagonal):
    lanes, row, column = packed_places()
    same = row == column
    upper = jnp.where(row > column, mixed, jnp.where(same, 0.5 * mixed, 0.0))
    lower = jnp.where(row < column, mixed, jnp.where(same, 0.5 * diagonal, 0.0))
    top, bottom = [], []
    for g in range(4):
        back = (128 - 32 * g) % 128
        top.append(jnp.where(lanes < 32, pltpu.roll(upper, back, 1), 0.0))
        left, right = pltpu.roll(corner, back, 1), pltpu.roll(lower, (back + 32) % 128, 1)
        bottom.append(jnp.where(lanes < 32, left, jnp.where(lanes < 64, right, 0.0)))
    half = jnp.concatenate(top + bottom, 0)[:, :K]
    return jnp.concatenate([jnp.zeros((K, K), F32), half + half.T], 1)


def selection(top, flipped):
    out = lax.broadcasted_iota(jnp.int32, (2 * BLOCK, 2 * BLOCK), 0)
    src = lax.broadcasted_iota(jnp.int32, (2 * BLOCK, 2 * BLOCK), 1)
    second = out >= BLOCK
    sensor = jnp.where(second, out - BLOCK, out)
    if flipped:
        sensor = BLOCK - 1 - sensor
    straight = jnp.where(second, 2 * sensor + 1, 2 * sensor)
    crossed = jnp.where(second, 2 * sensor, 2 * sensor + 1)
    minus = second if not flipped else jnp.logical_not(second)
    upper = jnp.where(src == straight, 1.0, 0.0)
    lower = jnp.where(src == crossed, jnp.where(minus, -1.0, 1.0), 0.0)
    return jnp.where(top, upper, lower).astype(BF16)


def music_kernel(
    own_any, tail_any, offs_ref, start_any, cov_ref, mapped_ref, gram_ref,
    own_ref, tail_ref, start_ref,
    got, picks, offs_all, offs_near, offs_now,
    row_w, row_m, col_w, col_m, acc,
    part1, land1, map1, part2, beside, middle, land2, sum2, part3, land3, sum3, partd, landd,
    wide_send, wide_recv, pair_send, pair_recv, near_send, near_recv, offs_send, offs_recv, local_sem,
    send_sem, recv_sem, ready,
):
    r = lax.axis_index("row")
    t = lax.axis_index("shift")
    x, y = lax.div(r, 8), lax.rem(r, 8)
    z, core = lax.div(t, 2), lax.rem(t, 2)
    rows, places = plane_peers(r), line_peers(t)
    column_rows = [x * 8 + lax.rem(y + b, 8) for b in (3, 5, 4, 2, 6, 1, 7)]
    bring_own = pltpu.make_async_copy(own_any, own_ref, local_sem.at[1])
    bring_own.start()
    barrier = pltpu.get_barrier_semaphore()
    across_rows = [lax.rem(x + d, 4) * 8 + y for d in (2, 1, 3)]
    signal_peers(barrier, column_rows + across_rows + [31 - r], places)

    @pl.when(r < ROWS - 1)
    def _():
        signal_peers(barrier, [r + 1], [])

    @pl.when((r >= 1) & (r != ROWS // 2))
    def _():
        signal_peers(barrier, [32 - r], [])

    bring_tail = pltpu.make_async_copy(tail_any, tail_ref, local_sem.at[2])
    bring_tail.start()
    bring_start = pltpu.make_async_copy(start_any, start_ref, local_sem.at[3])
    bring_start.start()

    lane = lax.broadcasted_iota(jnp.int32, (1, BLOCK), 1)
    offs_near[...] = jnp.where(lane == 0, offs_ref[0], jnp.where(lane == 1, offs_ref[1], offs_ref[2]))
    half = pl.ds(pl.multiple_of(core * BLOCK, BLOCK), BLOCK)
    other = pl.ds(pl.multiple_of((1 - core) * BLOCK, BLOCK), BLOCK)
    piece = pl.ds(pl.multiple_of(t * 16, 16), 16)
    bring_own.wait()
    extra = jnp.where(r >= 1, 1, 0) + jnp.where((r >= 1) & (r != ROWS // 2), 1, 0)
    pl.semaphore_wait(barrier, 11 + COLS - 1 + extra)
    signal_peers(ready, across_rows, [])

    slots = []
    for group in range(2):
        if group == 0:
            blocks = (4 * z + 2, 2 * t + 1, 4 * z + 4 * core)
        else:
            blocks = (30 - 4 * z, 31 - 2 * t, 32 - 4 * z - 4 * core)
        for place, block in enumerate(blocks):
            inside = block < ROWS
            bx, by = lax.div(block, 8), lax.rem(block, 8)
            source = block == r
            column = inside & (x == bx) & (y != by)
            opposite = inside & (x == lax.rem(bx + 2, 4)) & (y == by)
            slots.append((3 + 3 * group + place, block, source, column, opposite))

    def shared(slot):
        return slot % 3 == 0

    def wide(slot, k, dest, from_own=False):
        src, dst = own_ref if from_own else got.at[slot], got.at[slot]
        if shared(slot):
            src, dst = src.at[half], dst.at[half]
        return pltpu.make_async_remote_copy(
            src_ref=src,
            dst_ref=dst,
            send_sem=wide_send.at[slot - 3, k],
            recv_sem=wide_recv.at[slot - 3],
            device_id={"row": dest},
            device_id_type=MESH,
        )

    def pair(slot, part):
        return pltpu.make_async_remote_copy(
            src_ref=got.at[slot, part],
            dst_ref=got.at[slot, part],
            send_sem=pair_send.at[slot // 3 - 1],
            recv_sem=pair_recv.at[slot // 3 - 1],
            device_id={"shift": t + 1 - 2 * core},
            device_id_type=MESH,
        )

    def along_y(slot, from_own=False):
        for i, dest in enumerate(column_rows):
            wide(slot, i, dest, from_own).start()

    def along_x(slot, from_own=False):
        wide(slot, 8, lax.rem(x + 1, 4) * 8 + y, from_own).start()
        wide(slot, 9, lax.rem(x + 3, 4) * 8 + y, from_own).start()

    for slot, block, source, column, opposite in slots:
        @pl.when(source)
        def _():
            wide(slot, 7, lax.rem(x + 2, 4) * 8 + y, True).start()
            along_y(slot, True)
            along_x(slot, True)

    def near(slot, dest):
        return pltpu.make_async_remote_copy(
            src_ref=own_ref.at[piece],
            dst_ref=got.at[slot, piece],
            send_sem=near_send.at[slot, 0],
            recv_sem=near_recv.at[slot, 0],
            device_id={"row": dest},
            device_id_type=MESH,
        )

    def pass_on(slot, part, dest):
        return pltpu.make_async_remote_copy(
            src_ref=got.at[slot, part],
            dst_ref=got.at[slot, part],
            send_sem=near_send.at[slot, 1],
            recv_sem=near_recv.at[slot, 1],
            device_id={"shift": dest},
            device_id_type=MESH,
        )

    sends_near = (r >= 1, None, (r >= 1) & (r != 16))
    gets_near = (r != 31, None, (r != 0) & (r != 16))

    def when(condition, body):
        if condition is None:
            body()
        else:
            pl.when(condition)(body)

    for slot, dest in enumerate((r - 1, 31 - r, 32 - r)):
        when(sends_near[slot], lambda: near(slot, dest).start())

    def offs_copy(dest):
        return pltpu.make_async_remote_copy(
            src_ref=offs_near,
            dst_ref=offs_all.at[t],
            send_sem=offs_send,
            recv_sem=offs_recv,
            device_id={"shift": dest},
            device_id_type=MESH,
        )

    for dest in places:
        offs_copy(dest).start()
    offs_all[t] = offs_near[...]

    picks[0] = selection(r < ROWS // 2, False)
    picks[1] = selection(r < ROWS // 2, True)
    picks[2] = selection(t < COLS // 2, False)
    picks[3] = selection(t < COLS // 2, True)
    acc[...] = jnp.zeros_like(acc)
    bring_tail.wait()
    bring_start.wait()

    for slot, block, source, column, opposite in slots:
        @pl.when(source)
        def _():
            got[slot] = own_ref[...]

    def from_tail(slot):
        def body():
            got[slot] = tail_ref[...]

        return body

    pl.when(r == 31)(from_tail(0))
    pl.when(r == 0)(from_tail(2))
    pl.when(t == 15)(from_tail(5))
    pl.when(t == 0)(from_tail(8))

    @pl.when(r == 16)
    def _():
        got[2] = own_ref[...]

    def put(window, pick, place, block):
        both = jnp.dot(picks[pick], block, preferred_element_type=F32) * HALF_ROOT
        span = pl.ds(pl.multiple_of(place * BLOCK, BLOCK), BLOCK)
        window[0, span, :] = both[:BLOCK]
        window[1, span, :] = both[BLOCK:]

    put(row_w, 0, 0, own_ref[...])

    for slot, block, source, column, opposite in slots:
        @pl.when(opposite)
        def _():
            wide(slot, 0, r).wait_recv()
            along_y(slot)

    for slot in range(3):
        def body():
            near(slot, r).wait_recv()

            for dest in places:
                pass_on(slot, piece, dest).start()

        when(gets_near[slot], body)

    for slot, block, source, column, opposite in [slots[i] for i in (1, 4, 0, 3, 2, 5)]:
        @pl.when(column)
        def _():
            wide(slot, 0, r).wait_recv()
            along_x(slot)

    for slot, block, source, column, opposite in slots:
        if shared(slot):
            waits = jnp.logical_not(source | column | opposite)
            pl.when(waits)(lambda: wide(slot, 0, r).wait_recv())
            pl.when(jnp.logical_not(source))(lambda: pair(slot, half).start())

    every_offs = offs_all.at[pl.ds(0, COLS - 1)]
    whole_offs = pltpu.make_async_remote_copy(
        src_ref=every_offs,
        dst_ref=every_offs,
        send_sem=offs_send,
        recv_sem=offs_recv,
        device_id={"row": r},
        device_id_type=MESH,
    )
    whole_offs.wait_recv()
    to_scalar = pltpu.make_async_copy(offs_all, offs_now, local_sem.at[0])
    to_scalar.start()

    many = pl.ds(0, 16 * (COLS - 1))
    for slot in range(3):
        when(gets_near[slot], lambda: pass_on(slot, many, t).wait_recv())
    put(row_w, 0, 1, got[0])
    put(row_m, 1, 0, got[2])
    put(row_m, 1, 1, got[1])

    for slot, block, source, column, opposite in slots:
        if not shared(slot):
            waits = (block < ROWS) & jnp.logical_not(source | column | opposite)
            pl.when(waits)(lambda: wide(slot, 0, r).wait_recv())
    put(col_w, 2, 1, got[4])
    put(col_m, 3, 1, got[7])
    put(col_w, 2, 2 * core, got[5])
    put(col_m, 3, 2 * core, got[8])
    for slot, block, source, column, opposite in slots:
        if shared(slot):
            pl.when(jnp.logical_not(source))(lambda: pair(slot, other).wait_recv())
    put(col_w, 2, 2 - 2 * core, got[3])
    put(col_m, 3, 2 - 2 * core, got[6])
    to_scalar.wait()

    def pairs(window, mirror, offset, count):
        parts = []
        for c in range(2):
            a = window[c, pl.ds(offset, count), :]
            b = mirror[c, pl.ds(BLOCK - offset, count), :]
            parts.append((a + b).astype(BF16))
        return parts

    def some(i, c):
        lhs, rhs = [], []
        for j in range(12):
            offset = offs_now[i * 4 + j // 3, 0, j % 3]
            lhs += pairs(row_w, row_m, offset, BLOCK)
            rhs += pairs(col_w, col_m, offset, 2 * BLOCK)
        acc[...] += lax.dot_general(
            jnp.concatenate(lhs, 1), jnp.concatenate(rhs, 1), (((1,), (1,)), ((), ())), preferred_element_type=F32
        )
        return c

    lax.fori_loop(0, 4, some, 0)
    cov = acc[...] * (1.0 / (SNAPS * SHIFTS))
    cov_ref[...] = cov

    first = jnp.dot(start_ref[...], cov, precision=HIGHEST, preferred_element_type=F32)
    for c in range(2):
        for a in range(16):
            part1[16 * c + a] = first[4 * a : 4 * a + 4, BLOCK * c : BLOCK * c + BLOCK]

    def copy(src, dst, phase, where):
        return pltpu.make_async_remote_copy(
            src_ref=src,
            dst_ref=dst,
            send_sem=send_sem.at[phase],
            recv_sem=recv_sem.at[phase],
            device_id=where,
            device_id_type=MESH,
        )

    def total(phase, buffer, count):
        every = buffer.at[pl.ds(0, count)]
        return copy(every, every, phase, {"row": r})

    pl.semaphore_wait(ready, 3)
    for dest in rows:
        copy(part1.at[dest], land1.at[r], 0, {"row": dest}).start()
    land1[r] = part1[r]
    total(0, land1, ROWS - 1).wait_recv()
    map1[r] = jnp.sum(land1[...], axis=0)

    for dest in rows:
        copy(map1.at[r], map1.at[r], 1, {"row": dest}).start()
    total(1, map1, ROWS - 1).wait_recv()
    mapped = jnp.concatenate(
        [jnp.concatenate([map1[16 * c + a] for a in range(16)], 0) for c in range(2)], 1
    )

    lanes = lax.broadcasted_iota(jnp.int32, (8, BLOCK), 1)
    gram1 = lax.dot_general(
        mapped, jnp.concatenate([mapped, mapped], 0), (((1,), (1,)), ((), ())), precision=HIGHEST, preferred_element_type=F32
    )
    second = lax.dot_general(
        mapped, cov_ref[...], (((1,), (1,)), ((), ())), precision=HIGHEST, preferred_element_type=F32
    )
    for h in range(2):
        for i in range(4):
            part2[h, i] = second[32 * h + 8 * i : 32 * h + 8 * i + 8]
        for i in range(2):
            a = 16 * h + 8 * i
            part2[h, 4 + i] = jnp.where(lanes < K, gram1[a : a + 8], gram1[32 + a : 40 + a])
    partner = {"shift": t + 1 - 2 * core}
    meet = copy(part2.at[1 - core], beside, 2, partner)
    meet.start()
    meet.wait_recv()
    middle[...] = part2[core] + beside[...]
    for b in far_first(8):
        if b:
            copy(middle, land2.at[z], 3, {"shift": lax.rem(z + b, 8) * 2 + core}).start()
    land2[z] = middle[...]
    total(3, land2, 7).wait_recv()
    sum2[core] = jnp.sum(land2[...], axis=0)
    swap = copy(sum2.at[core], sum2.at[core], 7, partner)
    swap.start()
    swap.wait_recv()
    tiles = [sum2[h, 4 + i] for h in range(2) for i in range(2)]
    gram1 = jnp.concatenate(
        [jnp.where(lanes < K, 0.0, pltpu.roll(tile, K, 1)) for tile in tiles]
        + [jnp.where(lanes < K, 0.0, tile) for tile in tiles],
        0,
    )
    factor1 = lower_inverse(gram1)
    product = jnp.concatenate([sum2[h, i] for h in range(2) for i in range(4)], 0)
    mapped2 = jnp.dot(factor1, product, precision=HIGHEST, preferred_element_type=F32)
    corner, mixed, diagonal = packed_gram(mapped2)
    part3[...] = jnp.where(core == 0, corner, mixed)
    partd[...] = diagonal
    for dest in rows:
        copy(part3, land3.at[r], 4, {"row": dest}).start()
    for dest in rows:
        copy(partd, landd.at[r], 6, {"row": dest}).start()
    land3[r] = part3[...]
    landd[r] = partd[...]
    total(4, land3, ROWS - 1).wait_recv()
    sum3[core] = jnp.sum(land3[...], axis=0)
    halves = copy(sum3.at[core], sum3.at[core], 5, {"shift": t + 1 - 2 * core})
    halves.start()
    total(6, landd, ROWS - 1).wait_recv()
    diagonal = jnp.broadcast_to(jnp.sum(landd[...], axis=0), (8, 128))
    halves.wait_recv()
    whole = unpacked_gram(sum3[0], sum3[1], diagonal)
    mapped_ref[...] = mapped2
    gram_ref[...] = whole

    for slot, block, source, column, opposite in slots:
        def drain(low, high):
            def done(k, c):
                wide(slot, k, r).wait_send()
                return c

            lax.fori_loop(low, high, done, 0)

        pl.when(source)(lambda: drain(0, 10))
        pl.when(column)(lambda: drain(8, 10))
        pl.when(opposite)(lambda: drain(0, 7))
        if shared(slot):
            pl.when(jnp.logical_not(source))(lambda: pair(slot, half).wait_send())
    for slot in range(3):
        when(sends_near[slot], lambda: near(slot, r).wait_send())
        when(gets_near[slot], lambda: pass_on(slot, many, t).wait_send())
    whole_offs.wait_send()
    total(0, land1, ROWS - 1).wait_send()
    total(1, map1, ROWS - 1).wait_send()
    meet.wait_send()
    total(3, land2, 7).wait_send()
    swap.wait_send()
    total(4, land3, ROWS - 1).wait_send()
    halves.wait_send()
    total(6, landd, ROWS - 1).wait_send()


def finish_kernel(cov_ref, mapped_ref, gram_ref, cov_out, basis_ref, sem):
    write = pltpu.make_async_copy(cov_ref, cov_out, sem)
    write.start()
    basis_ref[...] = jnp.dot(
        lower_inverse(gram_ref[...]), mapped_ref[...], precision=HIGHEST, preferred_element_type=F32
    )
    write.wait()


def per_device(snapshots, tail_sensors, shift_offsets, start_basis):
    own = snapshots.reshape(2 * BLOCK, SNAPS)
    tail = tail_sensors.reshape(2 * BLOCK, SNAPS)
    vmem = pl.BlockSpec(memory_space=pltpu.VMEM)
    smem = pl.BlockSpec(memory_space=pltpu.SMEM)
    hbm = pl.BlockSpec(memory_space=pl.ANY)
    dma = pltpu.SemaphoreType.DMA
    f32 = lambda *shape: pltpu.VMEM(shape, F32)
    cov, mapped, gram = pl.pallas_call(
        music_kernel,
        out_shape=(
            pltpu.VMEM((BLOCK, 2 * BLOCK), F32),
            pltpu.VMEM((K, BLOCK), F32),
            pltpu.VMEM((K, BLOCK), F32),
        ),
        in_specs=[hbm, hbm, smem, hbm],
        out_specs=(vmem, vmem, vmem),
        scratch_shapes=[
            pltpu.VMEM((256, 128), BF16), pltpu.VMEM((256, 128), BF16), f32(K, BLOCK),
            pltpu.VMEM((9, 256, 128), BF16), pltpu.VMEM((4, 256, 256), BF16),
            pltpu.VMEM((COLS, 1, BLOCK), jnp.int32), pltpu.VMEM((1, BLOCK), jnp.int32),
            pltpu.SMEM((COLS, 1, BLOCK), jnp.int32),
            f32(2, 256, 128), f32(2, 256, 128), f32(2, 384, 128), f32(2, 384, 128), f32(128, 256),
            f32(32, 4, 128), f32(32, 4, 128), f32(32, 4, 128),
            f32(2, 6, 8, 128), f32(6, 8, 128), f32(6, 8, 128), f32(8, 6, 8, 128), f32(2, 6, 8, 128),
            f32(8, 128), f32(32, 8, 128), f32(2, 8, 128), f32(1, 128), f32(32, 1, 128),
            dma((6, 10)), dma((6,)), dma((2,)), dma((2,)), dma((3, 2)), dma((3, 2)), dma, dma, dma((4,)),
            dma((8,)), dma((8,)), pltpu.SemaphoreType.REGULAR,
        ],
        compiler_params=pltpu.CompilerParams(collective_id=0, has_side_effects=True),
        name="music",
    )(own, tail, shift_offsets, start_basis)
    return pl.pallas_call(
        finish_kernel,
        out_shape=(
            jax.ShapeDtypeStruct((BLOCK, 2 * BLOCK), F32),
            jax.ShapeDtypeStruct((K, BLOCK), F32),
        ),
        in_specs=[vmem, vmem, vmem],
        out_specs=(hbm, vmem),
        scratch_shapes=[dma],
        name="finish",
    )(*(pltpu.with_memory_space_constraint(x, pltpu.VMEM) for x in (cov, mapped, gram)))


def solution(mesh):
    in_specs = (P("row", None, None), P(), P("shift"), P(None, "row"))
    out_specs = (P("row", "shift"), P(None, "row"))
    return jax.shard_map(per_device, mesh=mesh, in_specs=in_specs, out_specs=out_specs, check_vma=False)
```

```python
import jax
import jax.numpy as jnp
from jax import lax
from jax.experimental import pallas as pl
from jax.experimental.pallas import tpu as pltpu
from jax.sharding import PartitionSpec as P

M = 4096
K = 64
SNAPS = 128
SHIFTS = 48
ROWS = 32
COLS = 16
BLOCK = 128
HALF_ROOT = 0.7071067811865476
MESH = pl.DeviceIdType.MESH
HIGHEST = lax.Precision.HIGHEST
F32 = jnp.float32
BF16 = jnp.bfloat16


def far_first(n):
    return sorted(range(n), key=lambda d: -min(d, n - d))


def plane_peers(r):
    x, y = lax.div(r, 8), lax.rem(r, 8)
    xs = [lax.rem(x + a, 4) * 8 for a in range(4)]
    ys = [lax.rem(y + b, 8) for b in range(8)]
    order = sorted(
        ((a, b) for a in range(4) for b in range(8) if a or b),
        key=lambda d: -min(d[0], 4 - d[0]) - min(d[1], 8 - d[1]),
    )
    return [xs[a] + ys[b] for a, b in order]


def line_peers(t):
    z, core = lax.div(t, 2), lax.rem(t, 2)
    zs = [lax.rem(z + a, 8) * 2 for a in range(8)]
    cores = [core, 1 - core]
    return [zs[a] + cores[b] for a in far_first(8) for b in (1, 0) if a or b]


def signal_peers(barrier, rows, places):
    for dest in rows:
        pl.semaphore_signal(barrier, inc=1, device_id={"row": dest}, device_id_type=MESH)
    for dest in places:
        pl.semaphore_signal(barrier, inc=1, device_id={"shift": dest}, device_id_type=MESH)


def lower_inverse(gram):
    lanes = lax.broadcasted_iota(jnp.int32, (8, 128), 1)
    subs = lax.broadcasted_iota(jnp.int32, (8, 128), 0)
    rows = [gram[8 * i : 8 * i + 8] + jnp.where(lanes == subs + 8 * i, 1.0, 0.0) for i in range(8)]
    out = []
    for b in range(8):
        cols = [
            {i: jnp.broadcast_to(rows[i][:, 64 + 8 * b + j : 65 + 8 * b + j], (8, 128)) for i in range(b, 8)}
            for j in range(8)
        ]
        scale = jnp.zeros((8, 128), F32)
        for l in range(8):
            cols[l][b] = jnp.where(lanes < 128 + subs, cols[l][b], 0.0)
        for j in range(8):
            root = jnp.broadcast_to(lax.rsqrt(cols[j][b])[j : j + 1], (8, 128))
            inverse = root * root
            scale = jnp.where(subs == j, root, scale)
            lead = jnp.broadcast_to(rows[b][j : j + 1], (8, 128))
            heads = {l: jnp.broadcast_to(cols[l][b][j : j + 1], (8, 128)) for l in range(j + 1, 8)}
            below = jnp.where(subs > j, cols[j][b], 0.0)
            for l in range(j + 1, 8):
                cols[l][b] = cols[l][b] - (below * heads[l]) * inverse
            rows[b] = rows[b] - (below * lead) * inverse
            for i in range(b + 1, 8):
                factor = cols[j][i] * inverse
                rows[i] = rows[i] - factor * lead
                for l in range(j + 1, 8):
                    cols[l][i] = cols[l][i] - factor * heads[l]
        out.append(rows[b] * scale)
    return jnp.concatenate(out, 0)[:, :64]


def packed_places():
    lanes = lax.broadcasted_iota(jnp.int32, (8, 128), 1)
    subs = lax.broadcasted_iota(jnp.int32, (8, 128), 0)
    group = sum(jnp.where(lanes >= 32 * g, 1, 0) for g in (1, 2, 3))
    return lanes, subs + 8 * group, lanes - 32 * group


def packed_gram(x):
    lanes, row, column = packed_places()

    def repeated(a, b):
        return lax.dot_general(
            a, jnp.concatenate([b] * 4, 0), (((1,), (1,)), ((), ())), precision=HIGHEST, preferred_element_type=F32
        )

    def packed(tiles):
        out = tiles[24:32]
        for g in (2, 1, 0):
            out = jnp.where(lanes < 32 * (g + 1), tiles[8 * g : 8 * g + 8], out)
        return out

    first, second = repeated(x, x[:32]), repeated(x[32:], x[32:])
    last = packed(second)
    mixed = jnp.where(row >= column, packed(first[:32]), last)
    return packed(first[32:]), mixed, jnp.sum(jnp.where(row == column, last, 0.0), axis=0, keepdims=True)


def unpacked_gram(corner, mixed, diagonal):
    lanes, row, column = packed_places()
    same = row == column
    upper = jnp.where(row > column, mixed, jnp.where(same, 0.5 * mixed, 0.0))
    lower = jnp.where(row < column, mixed, jnp.where(same, 0.5 * diagonal, 0.0))
    top, bottom = [], []
    for g in range(4):
        back = (128 - 32 * g) % 128
        top.append(jnp.where(lanes < 32, pltpu.roll(upper, back, 1), 0.0))
        left, right = pltpu.roll(corner, back, 1), pltpu.roll(lower, (back + 32) % 128, 1)
        bottom.append(jnp.where(lanes < 32, left, jnp.where(lanes < 64, right, 0.0)))
    half = jnp.concatenate(top + bottom, 0)[:, :K]
    return jnp.concatenate([jnp.zeros((K, K), F32), half + half.T], 1)


def selection(top, flipped):
    out = lax.broadcasted_iota(jnp.int32, (2 * BLOCK, 2 * BLOCK), 0)
    src = lax.broadcasted_iota(jnp.int32, (2 * BLOCK, 2 * BLOCK), 1)
    second = out >= BLOCK
    sensor = jnp.where(second, out - BLOCK, out)
    if flipped:
        sensor = BLOCK - 1 - sensor
    straight = jnp.where(second, 2 * sensor + 1, 2 * sensor)
    crossed = jnp.where(second, 2 * sensor, 2 * sensor + 1)
    minus = second if not flipped else jnp.logical_not(second)
    upper = jnp.where(src == straight, 1.0, 0.0)
    lower = jnp.where(src == crossed, jnp.where(minus, -1.0, 1.0), 0.0)
    return jnp.where(top, upper, lower).astype(BF16)


def music_kernel(
    own_any, tail_any, offs_ref, start_any, cov_ref, mapped_ref, gram_ref,
    own_ref, tail_ref, start_ref,
    got, picks, offs_all, offs_near, offs_now,
    row_w, row_m, col_w, col_m, acc,
    part1, land1, map1, part2, beside, middle, land2, sum2, part3, land3, sum3, partd, landd,
    wide_send, wide_recv, pair_send, pair_recv, near_send, near_recv, offs_send, offs_recv, local_sem,
    send_sem, recv_sem, ready,
):
    r = lax.axis_index("row")
    t = lax.axis_index("shift")
    x, y = lax.div(r, 8), lax.rem(r, 8)
    z, core = lax.div(t, 2), lax.rem(t, 2)
    rows, places = plane_peers(r), line_peers(t)
    column_rows = [x * 8 + lax.rem(y + b, 8) for b in (3, 5, 4, 2, 6, 1, 7)]
    bring_own = pltpu.make_async_copy(own_any, own_ref, local_sem.at[1])
    bring_own.start()
    barrier = pltpu.get_barrier_semaphore()
    across_rows = [lax.rem(x + d, 4) * 8 + y for d in (2, 1, 3)]
    signal_peers(barrier, column_rows + across_rows + [31 - r], places)

    @pl.when(r < ROWS - 1)
    def _():
        signal_peers(barrier, [r + 1], [])

    @pl.when((r >= 1) & (r != ROWS // 2))
    def _():
        signal_peers(barrier, [32 - r], [])

    bring_tail = pltpu.make_async_copy(tail_any, tail_ref, local_sem.at[2])
    bring_tail.start()
    bring_start = pltpu.make_async_copy(start_any, start_ref, local_sem.at[3])
    bring_start.start()

    lane = lax.broadcasted_iota(jnp.int32, (1, BLOCK), 1)
    offs_near[...] = jnp.where(lane == 0, offs_ref[0], jnp.where(lane == 1, offs_ref[1], offs_ref[2]))
    half = pl.ds(pl.multiple_of(core * BLOCK, BLOCK), BLOCK)
    other = pl.ds(pl.multiple_of((1 - core) * BLOCK, BLOCK), BLOCK)
    piece = pl.ds(pl.multiple_of(t * 16, 16), 16)
    bring_own.wait()
    extra = jnp.where(r >= 1, 1, 0) + jnp.where((r >= 1) & (r != ROWS // 2), 1, 0)
    pl.semaphore_wait(barrier, 11 + COLS - 1 + extra)
    signal_peers(ready, across_rows, [])

    slots = []
    for group in range(2):
        if group == 0:
            blocks = (4 * z + 2, 2 * t + 1, 4 * z + 4 * core)
        else:
            blocks = (30 - 4 * z, 31 - 2 * t, 32 - 4 * z - 4 * core)
        for place, block in enumerate(blocks):
            inside = block < ROWS
            bx, by = lax.div(block, 8), lax.rem(block, 8)
            source = block == r
            column = inside & (x == bx) & (y != by)
            opposite = inside & (x == lax.rem(bx + 2, 4)) & (y == by)
            slots.append((3 + 3 * group + place, block, source, column, opposite))

    def shared(slot):
        return slot % 3 == 0

    def wide(slot, k, dest, from_own=False):
        src, dst = own_ref if from_own else got.at[slot], got.at[slot]
        if shared(slot):
            src, dst = src.at[half], dst.at[half]
        return pltpu.make_async_remote_copy(
            src_ref=src,
            dst_ref=dst,
            send_sem=wide_send.at[slot - 3, k],
            recv_sem=wide_recv.at[slot - 3],
            device_id={"row": dest},
            device_id_type=MESH,
        )

    def pair(slot, part):
        return pltpu.make_async_remote_copy(
            src_ref=got.at[slot, part],
            dst_ref=got.at[slot, part],
            send_sem=pair_send.at[slot // 3 - 1],
            recv_sem=pair_recv.at[slot // 3 - 1],
            device_id={"shift": t + 1 - 2 * core},
            device_id_type=MESH,
        )

    def along_y(slot, from_own=False):
        for i, dest in enumerate(column_rows):
            wide(slot, i, dest, from_own).start()

    def along_x(slot, from_own=False):
        wide(slot, 8, lax.rem(x + 1, 4) * 8 + y, from_own).start()
        wide(slot, 9, lax.rem(x + 3, 4) * 8 + y, from_own).start()

    for slot, block, source, column, opposite in slots:
        @pl.when(source)
        def _():
            wide(slot, 7, lax.rem(x + 2, 4) * 8 + y, True).start()
            along_y(slot, True)
            along_x(slot, True)

    def near(slot, dest):
        return pltpu.make_async_remote_copy(
            src_ref=own_ref.at[piece],
            dst_ref=got.at[slot, piece],
            send_sem=near_send.at[slot, 0],
            recv_sem=near_recv.at[slot, 0],
            device_id={"row": dest},
            device_id_type=MESH,
        )

    def pass_on(slot, part, dest):
        return pltpu.make_async_remote_copy(
            src_ref=got.at[slot, part],
            dst_ref=got.at[slot, part],
            send_sem=near_send.at[slot, 1],
            recv_sem=near_recv.at[slot, 1],
            device_id={"shift": dest},
            device_id_type=MESH,
        )

    sends_near = (r >= 1, None, (r >= 1) & (r != 16))
    gets_near = (r != 31, None, (r != 0) & (r != 16))

    def when(condition, body):
        if condition is None:
            body()
        else:
            pl.when(condition)(body)

    for slot, dest in enumerate((r - 1, 31 - r, 32 - r)):
        when(sends_near[slot], lambda: near(slot, dest).start())

    def offs_copy(dest):
        return pltpu.make_async_remote_copy(
            src_ref=offs_near,
            dst_ref=offs_all.at[t],
            send_sem=offs_send,
            recv_sem=offs_recv,
            device_id={"shift": dest},
            device_id_type=MESH,
        )

    for dest in places:
        offs_copy(dest).start()
    offs_all[t] = offs_near[...]

    picks[0] = selection(r < ROWS // 2, False)
    picks[1] = selection(r < ROWS // 2, True)
    picks[2] = selection(t < COLS // 2, False)
    picks[3] = selection(t < COLS // 2, True)
    acc[...] = jnp.zeros_like(acc)
    bring_tail.wait()
    bring_start.wait()

    for slot, block, source, column, opposite in slots:
        @pl.when(source)
        def _():
            got[slot] = own_ref[...]

    def from_tail(slot):
        def body():
            got[slot] = tail_ref[...]

        return body

    pl.when(r == 31)(from_tail(0))
    pl.when(r == 0)(from_tail(2))
    pl.when(t == 15)(from_tail(5))
    pl.when(t == 0)(from_tail(8))

    @pl.when(r == 16)
    def _():
        got[2] = own_ref[...]

    def put(window, pick, place, block):
        both = jnp.dot(picks[pick], block, preferred_element_type=F32) * HALF_ROOT
        span = pl.ds(pl.multiple_of(place * BLOCK, BLOCK), BLOCK)
        window[0, span, :] = both[:BLOCK]
        window[1, span, :] = both[BLOCK:]

    put(row_w, 0, 0, own_ref[...])

    for slot, block, source, column, opposite in slots:
        @pl.when(opposite)
        def _():
            wide(slot, 0, r).wait_recv()
            along_y(slot)

    for slot in range(3):
        def body():
            near(slot, r).wait_recv()

            for dest in places:
                pass_on(slot, piece, dest).start()

        when(gets_near[slot], body)

    for slot, block, source, column, opposite in [slots[i] for i in (1, 4, 0, 3, 2, 5)]:
        @pl.when(column)
        def _():
            wide(slot, 0, r).wait_recv()
            along_x(slot)

    for slot, block, source, column, opposite in slots:
        if shared(slot):
            waits = jnp.logical_not(source | column | opposite)
            pl.when(waits)(lambda: wide(slot, 0, r).wait_recv())
            pl.when(jnp.logical_not(source))(lambda: pair(slot, half).start())

    every_offs = offs_all.at[pl.ds(0, COLS - 1)]
    whole_offs = pltpu.make_async_remote_copy(
        src_ref=every_offs,
        dst_ref=every_offs,
        send_sem=offs_send,
        recv_sem=offs_recv,
        device_id={"row": r},
        device_id_type=MESH,
    )
    whole_offs.wait_recv()
    to_scalar = pltpu.make_async_copy(offs_all, offs_now, local_sem.at[0])
    to_scalar.start()

    many = pl.ds(0, 16 * (COLS - 1))
    for slot in range(3):
        when(gets_near[slot], lambda: pass_on(slot, many, t).wait_recv())
    put(row_w, 0, 1, got[0])
    put(row_m, 1, 0, got[2])
    put(row_m, 1, 1, got[1])

    for slot, block, source, column, opposite in slots:
        if not shared(slot):
            waits = (block < ROWS) & jnp.logical_not(source | column | opposite)
            pl.when(waits)(lambda: wide(slot, 0, r).wait_recv())
    put(col_w, 2, 1, got[4])
    put(col_m, 3, 1, got[7])
    put(col_w, 2, 2 * core, got[5])
    put(col_m, 3, 2 * core, got[8])
    for slot, block, source, column, opposite in slots:
        if shared(slot):
            pl.when(jnp.logical_not(source))(lambda: pair(slot, other).wait_recv())
    put(col_w, 2, 2 - 2 * core, got[3])
    put(col_m, 3, 2 - 2 * core, got[6])
    to_scalar.wait()

    def pairs(window, mirror, offset, count):
        parts = []
        for c in range(2):
            a = window[c, pl.ds(offset, count), :]
            b = mirror[c, pl.ds(BLOCK - offset, count), :]
            parts.append((a + b).astype(BF16))
        return parts

    def some(i, c):
        lhs, rhs = [], []
        for j in range(24):
            offset = offs_now[i * 8 + j // 3, 0, j % 3]
            lhs += pairs(row_w, row_m, offset, BLOCK)
            rhs += pairs(col_w, col_m, offset, 2 * BLOCK)
        acc[...] += lax.dot_general(
            jnp.concatenate(lhs, 1), jnp.concatenate(rhs, 1), (((1,), (1,)), ((), ())), preferred_element_type=F32
        )
        return c

    lax.fori_loop(0, 2, some, 0)
    cov = acc[...] * (1.0 / (SNAPS * SHIFTS))
    cov_ref[...] = cov

    first = jnp.dot(start_ref[...], cov, precision=HIGHEST, preferred_element_type=F32)
    for c in range(2):
        for a in range(16):
            part1[16 * c + a] = first[4 * a : 4 * a + 4, BLOCK * c : BLOCK * c + BLOCK]

    def copy(src, dst, phase, where):
        return pltpu.make_async_remote_copy(
            src_ref=src,
            dst_ref=dst,
            send_sem=send_sem.at[phase],
            recv_sem=recv_sem.at[phase],
            device_id=where,
            device_id_type=MESH,
        )

    def total(phase, buffer, count):
        every = buffer.at[pl.ds(0, count)]
        return copy(every, every, phase, {"row": r})

    pl.semaphore_wait(ready, 3)
    for dest in rows:
        copy(part1.at[dest], land1.at[r], 0, {"row": dest}).start()
    land1[r] = part1[r]
    total(0, land1, ROWS - 1).wait_recv()
    map1[r] = jnp.sum(land1[...], axis=0)

    for dest in rows:
        copy(map1.at[r], map1.at[r], 1, {"row": dest}).start()
    total(1, map1, ROWS - 1).wait_recv()
    mapped = jnp.concatenate(
        [jnp.concatenate([map1[16 * c + a] for a in range(16)], 0) for c in range(2)], 1
    )

    lanes = lax.broadcasted_iota(jnp.int32, (8, BLOCK), 1)
    gram1 = lax.dot_general(
        mapped, jnp.concatenate([mapped, mapped], 0), (((1,), (1,)), ((), ())), precision=HIGHEST, preferred_element_type=F32
    )
    second = lax.dot_general(
        mapped, cov_ref[...], (((1,), (1,)), ((), ())), precision=HIGHEST, preferred_element_type=F32
    )
    for h in range(2):
        for i in range(4):
            part2[h, i] = second[32 * h + 8 * i : 32 * h + 8 * i + 8]
        for i in range(2):
            a = 16 * h + 8 * i
            part2[h, 4 + i] = jnp.where(lanes < K, gram1[a : a + 8], gram1[32 + a : 40 + a])
    partner = {"shift": t + 1 - 2 * core}
    meet = copy(part2.at[1 - core], beside, 2, partner)
    meet.start()
    meet.wait_recv()
    middle[...] = part2[core] + beside[...]
    for b in far_first(8):
        if b:
            copy(middle, land2.at[z], 3, {"shift": lax.rem(z + b, 8) * 2 + core}).start()
    land2[z] = middle[...]
    total(3, land2, 7).wait_recv()
    sum2[core] = jnp.sum(land2[...], axis=0)
    swap = copy(sum2.at[core], sum2.at[core], 7, partner)
    swap.start()
    swap.wait_recv()
    tiles = [sum2[h, 4 + i] for h in range(2) for i in range(2)]
    gram1 = jnp.concatenate(
        [jnp.where(lanes < K, 0.0, pltpu.roll(tile, K, 1)) for tile in tiles]
        + [jnp.where(lanes < K, 0.0, tile) for tile in tiles],
        0,
    )
    factor1 = lower_inverse(gram1)
    product = jnp.concatenate([sum2[h, i] for h in range(2) for i in range(4)], 0)
    mapped2 = jnp.dot(factor1, product, precision=HIGHEST, preferred_element_type=F32)
    corner, mixed, diagonal = packed_gram(mapped2)
    part3[...] = jnp.where(core == 0, corner, mixed)
    partd[...] = diagonal
    for dest in rows:
        copy(part3, land3.at[r], 4, {"row": dest}).start()
    for dest in rows:
        copy(partd, landd.at[r], 6, {"row": dest}).start()
    land3[r] = part3[...]
    landd[r] = partd[...]
    total(4, land3, ROWS - 1).wait_recv()
    sum3[core] = jnp.sum(land3[...], axis=0)
    halves = copy(sum3.at[core], sum3.at[core], 5, {"shift": t + 1 - 2 * core})
    halves.start()
    total(6, landd, ROWS - 1).wait_recv()
    diagonal = jnp.broadcast_to(jnp.sum(landd[...], axis=0), (8, 128))
    halves.wait_recv()
    whole = unpacked_gram(sum3[0], sum3[1], diagonal)
    mapped_ref[...] = mapped2
    gram_ref[...] = whole

    for slot, block, source, column, opposite in slots:
        def drain(low, high):
            def done(k, c):
                wide(slot, k, r).wait_send()
                return c

            lax.fori_loop(low, high, done, 0)

        pl.when(source)(lambda: drain(0, 10))
        pl.when(column)(lambda: drain(8, 10))
        pl.when(opposite)(lambda: drain(0, 7))
        if shared(slot):
            pl.when(jnp.logical_not(source))(lambda: pair(slot, half).wait_send())
    for slot in range(3):
        when(sends_near[slot], lambda: near(slot, r).wait_send())
        when(gets_near[slot], lambda: pass_on(slot, many, t).wait_send())
    whole_offs.wait_send()
    total(0, land1, ROWS - 1).wait_send()
    total(1, map1, ROWS - 1).wait_send()
    meet.wait_send()
    total(3, land2, 7).wait_send()
    swap.wait_send()
    total(4, land3, ROWS - 1).wait_send()
    halves.wait_send()
    total(6, landd, ROWS - 1).wait_send()


def finish_kernel(cov_ref, mapped_ref, gram_ref, cov_out, basis_ref, sem):
    write = pltpu.make_async_copy(cov_ref, cov_out, sem)
    write.start()
    basis_ref[...] = jnp.dot(
        lower_inverse(gram_ref[...]), mapped_ref[...], precision=HIGHEST, preferred_element_type=F32
    )
    write.wait()


def per_device(snapshots, tail_sensors, shift_offsets, start_basis):
    own = snapshots.reshape(2 * BLOCK, SNAPS)
    tail = tail_sensors.reshape(2 * BLOCK, SNAPS)
    vmem = pl.BlockSpec(memory_space=pltpu.VMEM)
    smem = pl.BlockSpec(memory_space=pltpu.SMEM)
    hbm = pl.BlockSpec(memory_space=pl.ANY)
    dma = pltpu.SemaphoreType.DMA
    f32 = lambda *shape: pltpu.VMEM(shape, F32)
    cov, mapped, gram = pl.pallas_call(
        music_kernel,
        out_shape=(
            pltpu.VMEM((BLOCK, 2 * BLOCK), F32),
            pltpu.VMEM((K, BLOCK), F32),
            pltpu.VMEM((K, BLOCK), F32),
        ),
        in_specs=[hbm, hbm, smem, hbm],
        out_specs=(vmem, vmem, vmem),
        scratch_shapes=[
            pltpu.VMEM((256, 128), BF16), pltpu.VMEM((256, 128), BF16), f32(K, BLOCK),
            pltpu.VMEM((9, 256, 128), BF16), pltpu.VMEM((4, 256, 256), BF16),
            pltpu.VMEM((COLS, 1, BLOCK), jnp.int32), pltpu.VMEM((1, BLOCK), jnp.int32),
            pltpu.SMEM((COLS, 1, BLOCK), jnp.int32),
            f32(2, 256, 128), f32(2, 256, 128), f32(2, 384, 128), f32(2, 384, 128), f32(128, 256),
            f32(32, 4, 128), f32(32, 4, 128), f32(32, 4, 128),
            f32(2, 6, 8, 128), f32(6, 8, 128), f32(6, 8, 128), f32(8, 6, 8, 128), f32(2, 6, 8, 128),
            f32(8, 128), f32(32, 8, 128), f32(2, 8, 128), f32(1, 128), f32(32, 1, 128),
            dma((6, 10)), dma((6,)), dma((2,)), dma((2,)), dma((3, 2)), dma((3, 2)), dma, dma, dma((4,)),
            dma((8,)), dma((8,)), pltpu.SemaphoreType.REGULAR,
        ],
        compiler_params=pltpu.CompilerParams(collective_id=0, has_side_effects=True),
        name="music",
    )(own, tail, shift_offsets, start_basis)
    return pl.pallas_call(
        finish_kernel,
        out_shape=(
            jax.ShapeDtypeStruct((BLOCK, 2 * BLOCK), F32),
            jax.ShapeDtypeStruct((K, BLOCK), F32),
        ),
        in_specs=[vmem, vmem, vmem],
        out_specs=(hbm, vmem),
        scratch_shapes=[dma],
        name="finish",
    )(*(pltpu.with_memory_space_constraint(x, pltpu.VMEM) for x in (cov, mapped, gram)))


def solution(mesh):
    in_specs = (P("row", None, None), P(), P("shift"), P(None, "row"))
    out_specs = (P("row", "shift"), P(None, "row"))
    return jax.shard_map(per_device, mesh=mesh, in_specs=in_specs, out_specs=out_specs, check_vma=False)
```
